256 devices in a mesh: section: 8 (over y, z_hi), mp: 32 (over x, z_lo, core).
Axes of the slice: x: 4, y: 4, z: 8 (z_hi: 2, z_lo: 4; z = z_hi * 4 + z_lo), core: 2. Of those that a mesh axis runs over, the one named last changes fastest.
Arguments:
- stream: bfloat16 [4096, 4096], P(('section', 'mp')), may hold values from -6 to 6
- ffn_gain: float32 [4096], replicated, may hold values from 0.25 to 1.75
- router_weight: bfloat16 [4096, 8], replicated, may hold values from -0.1875 to 0.1875
- expert_ids: int32 [4096, 2], P(('section', 'mp')), may hold values from 0 to 7, all different within a row; in each aligned block of 16 rows (0 to 15, 16 to 31, ...) at most 6 rows name the same one
- w_gate: bfloat16 [8, 4096, 14336], P('section', None, 'mp'), may hold values from -0.09375 to 0.09375
- w_up: bfloat16 [8, 4096, 14336], P('section', None, 'mp'), may hold values from -0.09375 to 0.09375
- w_down: bfloat16 [8, 14336, 4096], P('section', 'mp'), may hold values from -0.09375 to 0.09375
- attn_gain: float32 [4096], replicated, may hold values from 0.25 to 1.75
- w_kv: bfloat16 [4096, 2048], P(None, 'mp'), may hold values from -0.09375 to 0.09375
Outputs:
- stream_out: bfloat16 [4096, 4096], P(('section', 'mp'))
- kv_decode: bfloat16 [4096, 2048], P('section', 'mp')
The draws below stay inside these ranges and needn't reach their ends.
Inputs may be any that keep to these rules, and one draw needn't show every extreme that they name: `expert_ids`: each row names two different experts. Among the rows of one device no expert is named more than 6 times, a bound that some block reaches.
All inputs are finite; a program needn't handle non-finite values.
Results may differ from the reference program's by a relative error of at most 0.02.
Values may be sent and summed in bfloat16 or wider, within the bound.
A program may use at most 128 MiB of HBM per device.

```python
import math
import jax
import jax.numpy as jnp
import numpy as np
from jax import lax

D = 4096
FF = 14336
TOK_DEV = 16
EXPERTS = 8
CAP = 6
KVW = 2048
TOKENS = 4096
N_MP = 32


def steps_of(key, shape, split, least, largest):
    factor_of = 1.0
    for axis_at, shards_of in split:
        draws = jax.random.uniform(jax.random.fold_in(jax.random.fold_in(key, 6), axis_at), (shards_of,), jnp.float32, least / len(split), largest / len(split))
        factor_of = factor_of * jnp.repeat(jnp.exp(draws), shape[axis_at] // shards_of).reshape((-1,) + (1,) * (len(shape) - 1 - axis_at))
    return factor_of


def deal_out(rng, own, number, rows, count, top, reach, skew):
    sequence = jax.random.permutation(rng, count)
    crowded, common = portions_of(count, rows * top, reach, skew, True), portions_of(count, rows * top, reach, skew, False)
    places = jnp.arange(count)

    def named(sizes, turn):
        used = int((sizes > 0).sum())
        fixed = max(1, used // 4)
        moved = fixed + (places - fixed + turn * (used - fixed)) % max(1, count - fixed)
        return jnp.zeros((count,), jnp.int32).at[sequence[jnp.where(places < fixed, places, moved)]].set(jnp.asarray(sizes, jnp.int32))

    sizes = jnp.where(number % 4 == 0, named(crowded, number // 4), named(common, number - number // 4 - 1))
    mixed = jax.random.permutation(jax.random.fold_in(own, 3), count)
    source_of, taker = mixed[0:count // 2 * 2:2], mixed[1:count // 2 * 2:2]
    margin = jnp.minimum(sizes[source_of] - 1, reach - sizes[taker]) // 2
    margin = jnp.where((source_of == sequence[0]) | (taker == sequence[0]) | (sizes[taker] == 0), 0, jnp.maximum(margin, 0))
    moved = jax.random.randint(jax.random.fold_in(own, 4), (count // 2,), 0, 1 << 20) % (margin + 1)
    sizes = sizes.at[source_of].add(-moved).at[taker].add(moved)
    items = jnp.searchsorted(jnp.cumsum(sizes), jnp.arange(rows * top), side="right").astype(jnp.int32)
    listing = items.reshape(top, rows).T
    listing = listing[jax.random.permutation(jax.random.fold_in(own, 1), rows)]
    turn = jax.random.randint(jax.random.fold_in(own, 2), (rows, 1), 0, top)
    return jnp.take_along_axis(listing, (jnp.arange(top)[None, :] + turn) % top, axis=1)


def portions_of(number_of, total, bound, lean, full):
    loads = [(1 << 20) // math.isqrt(rank ** lean) + 1 for rank in range(1, number_of + 1)]
    largest = bound if full else min(bound, max(-(-total // number_of), total * loads[0] // sum(loads)))
    least = 1 if total - largest >= number_of - 1 else 0
    holding, spare = [largest] + [least] * (number_of - 1), total - largest - least * (number_of - 1)
    while spare > 0:
        free = [i for i in range(1, number_of) if holding[i] < largest] or [i for i in range(1, number_of) if holding[i] < bound]
        mass, left = sum([loads[i] for i in free]), spare
        for i in free:
            extra = min(bound - holding[i], max(1, left * loads[i] // mass), spare)
            holding[i] = holding[i] + extra
            spare = spare - extra
    return np.array(holding)


def normal_values(key, extent, scale, limit, cuts=(), kind=jnp.bfloat16):
    entries = jax.random.normal(key, extent, jnp.float32) * scale
    if len(cuts) > 0:
        entries = steps_of(key, extent, cuts, -0.22, 0.18) * entries
    return jnp.clip(entries, min=-limit, max=limit).astype(kind)


def setup_inputs(seed: int = 0) -> dict:
    keys = jax.random.split(jax.random.key(seed), 10)
    stream = normal_values(keys[0], (TOKENS, D), 1.0, 6.0, ((0, 256),))
    ffn_gain = jnp.clip(1.0 + 0.15 * jax.random.normal(keys[1], (D,), jnp.float32), 0.25, 1.75)
    router_weight = normal_values(keys[2], (D, EXPERTS), (D // 4) ** -0.5, 0.1875)
    expert_ids_keys = jax.random.split(jax.random.fold_in(keys[3], 1), TOKENS // TOK_DEV)
    expert_ids_turns = jax.random.permutation(jax.random.fold_in(keys[3], 3), TOKENS // TOK_DEV)
    expert_ids = jax.vmap(lambda own, number: deal_out(jax.random.fold_in(keys[3], 2), own, number, TOK_DEV, EXPERTS, 2, CAP, 2))(expert_ids_keys, expert_ids_turns).reshape((TOKENS, 2))
    w_gate = normal_values(keys[4], (EXPERTS, D, FF), D ** -0.5, 0.09375, ((0, 8), (2, 32)))
    w_up = normal_values(keys[5], (EXPERTS, D, FF), D ** -0.5, 0.09375, ((0, 8), (2, 32)))
    w_down = normal_values(keys[6], (EXPERTS, FF, D), (FF // 4) ** -0.5, 0.09375, ((0, 8), (1, 32)))
    attn_gain = jnp.clip(1.0 + 0.15 * jax.random.normal(keys[7], (D,), jnp.float32), 0.25, 1.75)
    w_kv = normal_values(keys[8], (D, KVW), D ** -0.5, 0.09375, ((1, 32),))
    return dict(stream=stream, ffn_gain=ffn_gain, router_weight=router_weight, expert_ids=expert_ids, w_gate=w_gate, w_up=w_up, w_down=w_down, attn_gain=attn_gain, w_kv=w_kv)


epsilon = 1e-05

def normalize(values, scale_gain):
    floats = values.astype(jnp.float32)
    return floats * lax.rsqrt(lax.optimization_barrier(jnp.mean(floats * floats, axis=-1, keepdims=True)) + epsilon) * scale_gain

def reference(stream, ffn_gain, router_weight, expert_ids, w_gate, w_up, w_down, attn_gain, w_kv):
    tokens = stream.shape[0]
    blocks = tokens // TOK_DEV
    normed = normalize(stream, ffn_gain).astype(jnp.bfloat16)
    logits = jnp.dot(normed, router_weight, preferred_element_type=jnp.float32)
    onehot = expert_ids[:, :, None] == jnp.arange(EXPERTS, dtype=jnp.int32)[None, None, :]
    chosen = lax.optimization_barrier(jnp.sum(jnp.where(onehot, logits[:, None, :], jnp.float32(0.0)), axis=-1))
    share_first = jax.nn.sigmoid(chosen[:, 0] - chosen[:, 1])
    flat_hits = onehot.reshape(blocks, TOK_DEV * 2, EXPERTS).astype(jnp.int32)
    before = jnp.cumsum(flat_hits, axis=1) - flat_hits
    slot_index = lax.optimization_barrier(jnp.sum(before * flat_hits, axis=-1)).reshape(tokens, 2)
    position = (jnp.arange(tokens, dtype=jnp.int32) // TOK_DEV)[:, None] * CAP + slot_index
    repeated = jnp.repeat(normed, 2, axis=0)
    block_width = FF // N_MP
    total = jnp.zeros((tokens, 2, D), jnp.float32)
    for expert in range(EXPERTS):
        target_index = jnp.where(expert_ids == expert, position, blocks * CAP).astype(jnp.int32)
        buffer = jnp.zeros((blocks * CAP, D), jnp.bfloat16).at[target_index.reshape(-1)].set(repeated, mode='drop')
        gate_part = jnp.dot(buffer, w_gate[expert], preferred_element_type=jnp.float32)
        up_part = jnp.dot(buffer, w_up[expert], preferred_element_type=jnp.float32)
        hidden = (jax.nn.silu(gate_part) * up_part).astype(jnp.bfloat16)
        hidden_blocks = hidden.reshape(blocks * CAP, N_MP, block_width).transpose(1, 0, 2)
        down_blocks = w_down[expert].reshape(N_MP, block_width, D)

        def add_block(carry, pair):
            product = jnp.dot(pair[0], pair[1], preferred_element_type=jnp.float32)
            rounded = lax.optimization_barrier(product.astype(jnp.bfloat16))
            return (carry + rounded.astype(jnp.float32), None)
        summed, unused = lax.scan(add_block, jnp.zeros((blocks * CAP, D), jnp.float32), (hidden_blocks, down_blocks))
        result_rows = summed.astype(jnp.bfloat16)
        safe_index = jnp.clip(target_index, 0, blocks * CAP - 1)
        picked = result_rows[safe_index.reshape(-1)].reshape(tokens, 2, D).astype(jnp.float32)
        total = total + jnp.where((expert_ids == expert)[:, :, None], picked, jnp.float32(0.0))
    updated = stream.astype(jnp.float32) + share_first[:, None] * total[:, 0] + (1.0 - share_first)[:, None] * total[:, 1]
    stream_out = updated.astype(jnp.bfloat16)
    attn_input = normalize(stream_out, attn_gain).astype(jnp.bfloat16)
    kv_local = jnp.dot(attn_input, w_kv, preferred_element_type=jnp.float32).astype(jnp.bfloat16)
    kv_decode = jnp.roll(kv_local, TOK_DEV * N_MP, axis=0)
    return (stream_out, kv_decode)
```

```python
import functools

import jax
import jax.numpy as jnp
from jax import lax
from jax.experimental import pallas as pl
from jax.experimental.pallas import tpu as pltpu
from jax.sharding import PartitionSpec as P

epsilon = 1e-05
MESH = pl.DeviceIdType.MESH
NX = 4
NZ = 4
VMEM_LIMIT = 66_000_000


def normalize(values, scale_gain):
    floats = values.astype(jnp.float32)
    return (
        floats * lax.rsqrt(jnp.mean(floats * floats, axis=-1, keepdims=True) + epsilon) * scale_gain
    )


class Place:
    def __init__(self):
        self.s = lax.axis_index("section")
        m = lax.axis_index("mp")
        self.x = m // (NZ * 2)
        self.z = (m // 2) % NZ
        self.c = m % 2
        z = self.z
        self.cols = [self.x, (self.x + 3) % NX, (self.x + 1) % NX, (self.x + 2) % NX]
        self.zs = [z, z + 1 - 2 * (z % 2), (z + 2) % NZ, NZ - 1 - z]

    def at(self, x, z, c):
        return (self.s, x * (NZ * 2) + z * 2 + c)

    def partner(self):
        return self.at(self.x, self.z, 1 - self.c)

    def side(self, way):
        return self.at(self.cols[2 - way], self.z, self.c)

    def zpeer(self, k):
        return self.at(self.x, self.zs[k], self.c)

    def peers(self):
        return [self.partner(), self.side(0), self.side(1)] + [self.zpeer(k) for k in (1, 2, 3)]


class Gather:
    def __init__(self, place, X, sems):
        self.p, self.X = place, X
        self.zs_s, self.zs_r, self.xs_s, self.xs_r, self.x2_s, self.x2_r, self.p_s, self.p_r = sems
        self.half = X.shape[-1] // 2

    @staticmethod
    def sems():
        dma = pltpu.SemaphoreType.DMA
        return [dma((3,)), dma((3,)), dma((2, 4)), dma((2, 4)), dma((2, 4)), dma((2, 4)), dma((4, 4)), dma((4, 4))]

    def block(self, r, q, c):
        return self.X.at[self.p.cols[r], self.p.zs[q], c]

    def copy(self, ref, send, recv, to):
        return pltpu.make_async_remote_copy(
            src_ref=ref, dst_ref=ref, send_sem=send, recv_sem=recv, device_id=to, device_id_type=MESH
        )

    def to_z(self, k):
        return self.copy(self.block(0, 0, self.p.c), self.zs_s.at[k - 1], self.zs_r.at[k - 1], self.p.zpeer(k))

    def from_z(self, k):
        return self.copy(self.block(0, k, self.p.c), self.zs_s.at[k - 1], self.zs_r.at[k - 1], self.p.zpeer(k))

    def to_x(self, way, q):
        return self.copy(self.block(0, q, self.p.c), self.xs_s.at[way, q], self.xs_r.at[way, q], self.p.side(way))

    def from_x(self, way, q):
        return self.copy(self.block(1 + way, q, self.p.c), self.xs_s.at[way, q], self.xs_r.at[way, q], self.p.side(way))

    def part(self, r, q, way):
        return self.X.at[self.p.cols[r], self.p.zs[q], self.p.c, :, pl.ds(way * self.half, self.half)]

    def on_x(self, way, q):
        return self.copy(self.part(1 + way, q, way), self.x2_s.at[way, q], self.x2_r.at[way, q], self.p.side(way))

    def from_x2(self, way, q):
        return self.copy(self.part(3, q, way), self.x2_s.at[way, q], self.x2_r.at[way, q], self.p.side(way))

    def pair(self, r, q):
        return self.copy(self.block(r, q, self.p.c), self.p_s.at[r, q], self.p_r.at[r, q], self.p.partner())

    def from_pair(self, r, q):
        return self.copy(self.block(r, q, 1 - self.p.c), self.p_s.at[r, q], self.p_r.at[r, q], self.p.partner())

    def start(self):
        self.to_x(0, 0).start()
        self.to_x(1, 0).start()
        for k in (1, 2, 3):
            self.to_z(k).start()
        self.pair(0, 0).start()

    def spread_z(self, k):
        self.from_z(k).wait_recv()
        self.to_x(0, k).start()
        self.to_x(1, k).start()
        self.pair(0, k).start()

    def spread_x(self, q):
        for way in (0, 1):
            self.from_x(way, q).wait_recv()
            self.on_x(way, q).start()
        for way in (0, 1):
            self.pair(1 + way, q).start()

    def spread_x2(self, q):
        for way in (0, 1):
            self.from_x2(way, q).wait_recv()
        self.pair(3, q).start()

    def need(self, r, qs):
        for q in qs:
            self.from_pair(r, q).wait_recv()

    def finish(self):
        for k in (1, 2, 3):
            self.to_z(k).wait_send()
        for q in range(4):
            for way in (0, 1):
                self.to_x(way, q).wait_send()
                self.on_x(way, q).wait_send()
            for r in range(4):
                self.pair(r, q).wait_send()


def enter(peers):
    barrier = pltpu.get_barrier_semaphore()
    for peer in peers:
        pl.semaphore_signal(barrier, inc=1, device_id=peer, device_id_type=MESH)
    pl.semaphore_wait(barrier, len(peers))


class Reduce:
    def __init__(self, place, Y, PR, RX, RH, RZ, sems):
        self.p, self.Y, self.PR, self.RX, self.RH, self.RZ = place, Y, PR, RX, RH, RZ
        self.py_s, self.py_r, self.h_s, self.h_r, self.w_s, self.w_r, self.rz_s, self.rz_r = sems
        self.half = Y.shape[-1] // 2

    @staticmethod
    def sems():
        dma = pltpu.SemaphoreType.DMA
        return [
            dma((4, 4)), dma((4, 4)), dma((2, 4)), dma((2, 4)), dma((2, 4, 2)), dma((2, 4, 2)), dma((3,)), dma((3,)),
        ]

    def copy(self, src, dst, send, recv, to):
        return pltpu.make_async_remote_copy(
            src_ref=src, dst_ref=dst, send_sem=send, recv_sem=recv, device_id=to, device_id_type=MESH
        )

    def pair(self, r, q):
        src = self.Y.at[self.p.cols[r], self.p.zs[q], 1 - self.p.c]
        return self.copy(src, self.PR.at[r, q], self.py_s.at[r, q], self.py_r.at[r, q], self.p.partner())

    def cols(self, n):
        return pl.ds(n * self.half, self.half)

    def through(self, way, q):
        src = self.Y.at[self.p.cols[3], self.p.zs[q], self.p.c, :, self.cols(1 - way)]
        return self.copy(src, self.RH.at[way, q], self.h_s.at[way, q], self.h_r.at[way, q], self.p.side(way))

    def beside(self, way, q, n):
        r = 2 - way
        src = self.Y.at[self.p.cols[r], self.p.zs[q], self.p.c, :, self.cols(n)]
        dst = self.RX.at[way, q, :, self.cols(n)]
        return self.copy(src, dst, self.w_s.at[way, q, n], self.w_r.at[way, q, n], self.p.side(way))

    def to_z(self, k):
        src = self.Y.at[self.p.cols[0], self.p.zs[k], self.p.c]
        return self.copy(src, self.RZ.at[k - 1], self.rz_s.at[k - 1], self.rz_r.at[k - 1], self.p.zpeer(k))

    def first(self, q):
        p = self.p
        for r in (3, 1, 2, 0):
            self.pair(r, q).wait_recv()
            at = (p.cols[r], p.zs[q], p.c)
            self.Y[at] = (self.Y[at].astype(jnp.float32) + self.PR[r, q].astype(jnp.float32)).astype(jnp.bfloat16)
            if r == 3:
                self.through(0, q).start()
                self.through(1, q).start()
            if r == 1:
                self.beside(1, q, 1).start()
            if r == 2:
                self.beside(0, q, 0).start()

    def second(self, q):
        p = self.p
        for way in (1, 0):
            n = 1 - way
            self.through(way, q).wait_recv()
            at = (p.cols[2 - way], p.zs[q], p.c, slice(None), self.cols(n))
            self.Y[at] = (self.Y[at].astype(jnp.float32) + self.RH[way, q].astype(jnp.float32)).astype(jnp.bfloat16)
            self.beside(way, q, n).start()

    def third(self, q):
        p = self.p
        for way in (0, 1):
            for n in (0, 1):
                self.beside(way, q, n).wait_recv()
        if q:
            at = (p.cols[0], p.zs[q], p.c)
            total = self.Y[at].astype(jnp.float32) + self.RX[0, q].astype(jnp.float32) + self.RX[1, q].astype(jnp.float32)
            self.Y[at] = total.astype(jnp.bfloat16)
            self.to_z(q).start()

    def total(self):
        p = self.p
        for k in (1, 2, 3):
            self.to_z(k).wait_recv()
        at = (p.cols[0], p.zs[0], p.c)
        total = self.Y[at].astype(jnp.float32) + self.RX[0, 0].astype(jnp.float32) + self.RX[1, 0].astype(jnp.float32)
        for k in range(3):
            total = total + self.RZ[k].astype(jnp.float32)
        return total

    def finish(self):
        for k in (1, 2, 3):
            self.to_z(k).wait_send()
        for q in range(4):
            for way in (0, 1):
                self.through(way, q).wait_send()
                for n in (0, 1):
                    self.beside(way, q, n).wait_send()
            for r in range(4):
                self.pair(r, q).wait_send()


def ffn_kernel(x_ref, wg_ref, wu_ref, wd_ref, out_ref, X, Y, WG, WU, WD, H, PR, RX, RH, RZ, local, *sems):
    p = Place()
    gather = Gather(p, X, sems[:8])
    reduce = Reduce(p, Y, PR, RX, RH, RZ, sems[8:])
    own = pltpu.make_async_copy(x_ref, gather.block(0, 0, p.c), local.at[0])
    loads = [
        pltpu.make_async_copy(ref.at[0], buf, local.at[1 + i])
        for i, (ref, buf) in enumerate(((wg_ref, WG), (wu_ref, WU), (wd_ref, WD)))
    ]
    own.start()
    for load in loads:
        load.start()
    enter(p.peers())
    own.wait()
    gather.start()
    gather.spread_z(1)
    rows = X.shape[-2]
    model = X.shape[-1]
    tile = min(512, model)
    order = ((0, 0), (1, 0), (2, 0), (0, 1), (3, 0), (1, 1), (2, 1), (3, 1))

    def before(i):
        if i == 0:
            gather.spread_x(0)
            for load in loads:
                load.wait()
        if i == 1:
            gather.spread_z(2)
            gather.spread_x(1)
        if i == 3:
            gather.spread_z(3)
        if i == 4:
            gather.spread_x2(0)
            gather.spread_x2(1)
            gather.spread_x(2)
        if i == 5:
            gather.spread_x(3)
        if i == 6:
            reduce.first(1)
        if i == 7:
            gather.spread_x2(2)
            gather.spread_x2(3)
            reduce.second(1)
        r, b = order[i]
        gather.need(r, (2 * b, 2 * b + 1))

    def after(i):
        r, b = order[i]
        for q in (2 * b, 2 * b + 1):
            reduce.pair(r, q).start()

    def step(i, carry):
        for n in range(8):
            pl.when(i == n)(functools.partial(before, n))
        r = (i == 1) * 1 + (i == 2) * 2 + (i == 4) * 3 + (i == 5) * 1 + (i == 6) * 2 + (i == 7) * 3
        b = (i == 3) * 1 + (i >= 5) * 1
        shift = (r == 1) * 3 + (r == 2) * 1 + (r == 3) * 2
        col = (p.x + shift) % NX
        pair = (p.z // 2 + b) % 2
        zs = pl.ds(2 * pair, 2)
        value = X[col, zs].reshape(4 * rows, model)
        gate = jnp.dot(value, WG[...], preferred_element_type=jnp.float32)
        up = jnp.dot(value, WU[...], preferred_element_type=jnp.float32)
        H[...] = (gate / (1.0 + jnp.exp(-gate)) * up).astype(jnp.bfloat16)

        def down(n, carry):
            at = pl.ds(pl.multiple_of(n * tile, tile), tile)
            part = jnp.dot(H[...], WD[:, at], preferred_element_type=jnp.float32)
            Y[col, zs, :, :, at] = part.astype(jnp.bfloat16).reshape(2, 2, rows, tile)
            return carry

        lax.fori_loop(0, model // tile, down, 0)
        for n in range(8):
            pl.when(i == n)(functools.partial(after, n))
        return carry

    lax.fori_loop(0, 8, step, 0)
    reduce.first(2)
    reduce.third(1)
    reduce.first(3)
    reduce.second(2)
    reduce.first(0)
    reduce.second(3)
    reduce.third(2)
    reduce.second(0)
    reduce.third(3)
    reduce.third(0)
    out_ref[...] = reduce.total().astype(jnp.bfloat16)
    gather.finish()
    reduce.finish()


def ffn(inbound, w_gate, w_up, w_down):
    rows, model = inbound.shape
    hidden = w_gate.shape[-1]
    bf16 = jnp.bfloat16
    any_space = pl.BlockSpec(memory_space=pl.ANY)
    return pl.pallas_call(
        ffn_kernel,
        out_shape=jax.ShapeDtypeStruct((rows, model), bf16),
        in_specs=[any_space] * 4,
        out_specs=pl.BlockSpec(memory_space=pltpu.VMEM),
        scratch_shapes=[
            pltpu.VMEM((NX, NZ, 2, rows, model), bf16),
            pltpu.VMEM((NX, NZ, 2, rows, model), bf16),
            pltpu.VMEM((model, hidden), bf16),
            pltpu.VMEM((model, hidden), bf16),
            pltpu.VMEM((hidden, model), bf16),
            pltpu.VMEM((4 * rows, hidden), bf16),
            pltpu.VMEM((4, 4, rows, model), bf16),
            pltpu.VMEM((2, 4, rows, model), bf16),
            pltpu.VMEM((2, 4, rows, model // 2), bf16),
            pltpu.VMEM((3, rows, model), bf16),
            pltpu.SemaphoreType.DMA((4,)),
            *Gather.sems(),
            *Reduce.sems(),
        ],
        compiler_params=pltpu.CompilerParams(
            collective_id=0, has_side_effects=True, vmem_limit_bytes=VMEM_LIMIT
        ),
        name="ffn",
    )(inbound, w_gate, w_up, w_down)


def kv_kernel(sections, x_ref, w_ref, out_ref, X, S, local, send, recv, *sems):
    p = Place()
    gather = Gather(p, X, sems)
    rows, model = X.shape[-2:]
    group = NZ * 2 * rows
    own = pltpu.make_async_copy(x_ref, gather.block(0, 0, p.c), local)
    own.start()
    m = lax.axis_index("mp")
    after = ((p.s + 1) % sections, m)
    ahead = ((p.s + sections - 1) % sections, m)
    enter(p.peers() + [after, ahead])
    own.wait()
    gather.start()

    def piece(r):
        at = pl.ds(pl.multiple_of(p.cols[r] * group, group), group)
        return pltpu.make_async_remote_copy(
            src_ref=S.at[p.cols[r]], dst_ref=out_ref.at[at], send_sem=send.at[r], recv_sem=recv.at[r],
            device_id=after, device_id_type=MESH,
        )

    def product(r):
        value = X[p.cols[r]].reshape(group, model)
        S[p.cols[r]] = jnp.dot(value, w_ref[...], preferred_element_type=jnp.float32).astype(jnp.bfloat16)
        piece(r).start()

    gather.spread_z(1)
    gather.spread_x(0)
    gather.spread_z(2)
    gather.spread_x(1)
    gather.spread_z(3)
    gather.spread_x(2)
    gather.need(0, range(4))
    product(0)
    gather.spread_x(3)
    gather.spread_x2(0)
    gather.spread_x2(1)
    gather.need(1, range(4))
    product(1)
    gather.need(2, range(4))
    product(2)
    gather.spread_x2(2)
    gather.spread_x2(3)
    gather.need(3, range(4))
    product(3)
    for r in range(4):
        piece(r).wait_recv()
    for r in range(4):
        piece(r).wait_send()
    gather.finish()


def kv_sent(attn_input, w_kv):
    rows, model = attn_input.shape
    width = w_kv.shape[1]
    bf16 = jnp.bfloat16
    vmem = pl.BlockSpec(memory_space=pltpu.VMEM)
    return pl.pallas_call(
        functools.partial(kv_kernel, lax.axis_size("section")),
        out_shape=jax.ShapeDtypeStruct((NX * NZ * 2 * rows, width), bf16),
        in_specs=[pl.BlockSpec(memory_space=pl.ANY), vmem],
        out_specs=vmem,
        scratch_shapes=[
            pltpu.VMEM((NX, NZ, 2, rows, model), bf16),
            pltpu.VMEM((NX, NZ * 2 * rows, width), bf16),
            pltpu.SemaphoreType.DMA,
            pltpu.SemaphoreType.DMA((4,)),
            pltpu.SemaphoreType.DMA((4,)),
            *Gather.sems(),
        ],
        compiler_params=pltpu.CompilerParams(
            collective_id=1, has_side_effects=True, vmem_limit_bytes=VMEM_LIMIT
        ),
        name="kv_sent",
    )(attn_input, w_kv)


def body(stream, ffn_gain, router_weight, expert_ids, w_gate, w_up, w_down, attn_gain, w_kv):
    own_rows = stream.shape[0]
    model_width = stream.shape[1]
    experts = router_weight.shape[1]
    capacity = min(own_rows, 3 * own_rows // experts)
    normed = normalize(stream, ffn_gain).astype(jnp.bfloat16)
    logits = jnp.dot(normed, router_weight, preferred_element_type=jnp.float32)
    onehot = expert_ids[:, :, None] == jnp.arange(experts, dtype=jnp.int32)[None, None, :]
    chosen = jnp.sum(jnp.where(onehot, logits[:, None, :], jnp.float32(0.0)), axis=-1)
    share_first = jax.nn.sigmoid(chosen[:, 0] - chosen[:, 1])
    flat_hits = onehot.reshape(own_rows * 2, experts).astype(jnp.int32)
    before = jnp.cumsum(flat_hits, axis=0) - flat_hits
    slot_index = jnp.sum(before * flat_hits, axis=-1)
    expert_flat = expert_ids.reshape(-1)
    route_table = (
        expert_flat[None, None, :] == jnp.arange(experts, dtype=jnp.int32)[:, None, None]
    ) & (slot_index[None, None, :] == jnp.arange(capacity, dtype=jnp.int32)[None, :, None])
    route_table = route_table.astype(jnp.bfloat16)
    repeated = jnp.repeat(normed, 2, axis=0)
    buffer = jnp.einsum(
        "ecr,rd->ecd", route_table, repeated, preferred_element_type=jnp.float32
    ).astype(jnp.bfloat16)
    arrived = lax.all_to_all(buffer, "section", split_axis=0, concat_axis=0, tiled=True)
    inbound = arrived.reshape(experts * capacity, model_width)
    summed = ffn(inbound, w_gate, w_up, w_down)
    results = summed.reshape(experts, capacity, model_width)
    returned = lax.all_to_all(results, "section", split_axis=0, concat_axis=0, tiled=True)
    picked = jnp.einsum("ecr,ecd->rd", route_table, returned, preferred_element_type=jnp.float32)
    picked = picked.reshape(own_rows, 2, model_width)
    updated = (
        stream.astype(jnp.float32)
        + share_first[:, None] * picked[:, 0]
        + (1.0 - share_first)[:, None] * picked[:, 1]
    )
    stream_out = updated.astype(jnp.bfloat16)
    attn_input = normalize(stream_out, attn_gain).astype(jnp.bfloat16)
    kv_decode = kv_sent(attn_input, w_kv)
    return (stream_out, kv_decode)


def solution(mesh):
    in_specs = (
        P(("section", "mp"), None),
        P(),
        P(),
        P(("section", "mp"), None),
        P("section", None, "mp"),
        P("section", None, "mp"),
        P("section", "mp", None),
        P(),
        P(None, "mp"),
    )
    out_specs = (P(("section", "mp"), None), P("section", "mp"))
    return jax.shard_map(body, mesh=mesh, in_specs=in_specs, out_specs=out_specs, check_vma=False)
```

```python
import functools

import jax
import jax.numpy as jnp
from jax import lax
from jax.experimental import pallas as pl
from jax.experimental.pallas import tpu as pltpu
from jax.sharding import PartitionSpec as P

epsilon = 1e-05
MESH = pl.DeviceIdType.MESH
NX = 4
NZ = 4
VMEM_LIMIT = 66_000_000


class Place:
    def __init__(self):
        self.s = lax.axis_index("section")
        m = lax.axis_index("mp")
        self.x = m // (NZ * 2)
        self.z = (m // 2) % NZ
        self.c = m % 2
        z = self.z
        self.cols = [self.x, (self.x + 3) % NX, (self.x + 1) % NX, (self.x + 2) % NX]
        self.zs = [z, z + 1 - 2 * (z % 2), (z + 2) % NZ, NZ - 1 - z]

    def at(self, x, z, c):
        return (self.s, x * (NZ * 2) + z * 2 + c)

    def partner(self):
        return self.at(self.x, self.z, 1 - self.c)

    def side(self, way):
        return self.at(self.cols[2 - way], self.z, self.c)

    def zpeer(self, k):
        return self.at(self.x, self.zs[k], self.c)

    def peers(self):
        return [self.partner(), self.side(0), self.side(1)] + [self.zpeer(k) for k in (1, 2, 3)]


class Gather:
    def __init__(self, place, X, sems):
        self.p, self.X = place, X
        self.zs_s, self.zs_r, self.xs_s, self.xs_r, self.x2_s, self.x2_r, self.p_s, self.p_r = sems
        self.half = X.shape[-1] // 2

    @staticmethod
    def sems():
        dma = pltpu.SemaphoreType.DMA
        return [dma((3,)), dma((3,)), dma((2, 4)), dma((2, 4)), dma((2, 4)), dma((2, 4)), dma((4, 4)), dma((4, 4))]

    def block(self, r, q, c):
        return self.X.at[self.p.cols[r], self.p.zs[q], c]

    def copy(self, ref, send, recv, to):
        return pltpu.make_async_remote_copy(
            src_ref=ref, dst_ref=ref, send_sem=send, recv_sem=recv, device_id=to, device_id_type=MESH
        )

    def to_z(self, k):
        return self.copy(self.block(0, 0, self.p.c), self.zs_s.at[k - 1], self.zs_r.at[k - 1], self.p.zpeer(k))

    def from_z(self, k):
        return self.copy(self.block(0, k, self.p.c), self.zs_s.at[k - 1], self.zs_r.at[k - 1], self.p.zpeer(k))

    def to_x(self, way, q):
        return self.copy(self.block(0, q, self.p.c), self.xs_s.at[way, q], self.xs_r.at[way, q], self.p.side(way))

    def from_x(self, way, q):
        return self.copy(self.block(1 + way, q, self.p.c), self.xs_s.at[way, q], self.xs_r.at[way, q], self.p.side(way))

    def part(self, r, q, way):
        return self.X.at[self.p.cols[r], self.p.zs[q], self.p.c, :, pl.ds(way * self.half, self.half)]

    def on_x(self, way, q):
        return self.copy(self.part(1 + way, q, way), self.x2_s.at[way, q], self.x2_r.at[way, q], self.p.side(way))

    def from_x2(self, way, q):
        return self.copy(self.part(3, q, way), self.x2_s.at[way, q], self.x2_r.at[way, q], self.p.side(way))

    def pair(self, r, q):
        return self.copy(self.block(r, q, self.p.c), self.p_s.at[r, q], self.p_r.at[r, q], self.p.partner())

    def from_pair(self, r, q):
        return self.copy(self.block(r, q, 1 - self.p.c), self.p_s.at[r, q], self.p_r.at[r, q], self.p.partner())

    def start(self):
        self.to_x(0, 0).start()
        self.to_x(1, 0).start()
        for k in (1, 2, 3):
            self.to_z(k).start()
        self.pair(0, 0).start()

    def spread_z(self, k):
        self.from_z(k).wait_recv()
        self.to_x(0, k).start()
        self.to_x(1, k).start()
        self.pair(0, k).start()

    def spread_x(self, q):
        for way in (0, 1):
            self.from_x(way, q).wait_recv()
            self.on_x(way, q).start()
        for way in (0, 1):
            self.pair(1 + way, q).start()

    def spread_x2(self, q):
        for way in (0, 1):
            self.from_x2(way, q).wait_recv()
        self.pair(3, q).start()

    def need(self, r, qs):
        for q in qs:
            self.from_pair(r, q).wait_recv()

    def finish(self):
        for k in (1, 2, 3):
            self.to_z(k).wait_send()
        for q in range(4):
            for way in (0, 1):
                self.to_x(way, q).wait_send()
                self.on_x(way, q).wait_send()
            for r in range(4):
                self.pair(r, q).wait_send()


def enter(peers):
    barrier = pltpu.get_barrier_semaphore()
    for peer in peers:
        pl.semaphore_signal(barrier, inc=1, device_id=peer, device_id_type=MESH)
    pl.semaphore_wait(barrier, len(peers))


class Reduce:
    def __init__(self, place, Y, PR, RX, RH, RZ, sems):
        self.p, self.Y, self.PR, self.RX, self.RH, self.RZ = place, Y, PR, RX, RH, RZ
        self.py_s, self.py_r, self.h_s, self.h_r, self.w_s, self.w_r, self.rz_s, self.rz_r = sems
        self.half = Y.shape[-1] // 2

    @staticmethod
    def sems():
        dma = pltpu.SemaphoreType.DMA
        return [
            dma((4, 4)), dma((4, 4)), dma((2, 4)), dma((2, 4)), dma((2, 4, 2)), dma((2, 4, 2)), dma((3,)), dma((3,)),
        ]

    def copy(self, src, dst, send, recv, to):
        return pltpu.make_async_remote_copy(
            src_ref=src, dst_ref=dst, send_sem=send, recv_sem=recv, device_id=to, device_id_type=MESH
        )

    def pair(self, r, q):
        src = self.Y.at[self.p.cols[r], self.p.zs[q], 1 - self.p.c]
        return self.copy(src, self.PR.at[r, q], self.py_s.at[r, q], self.py_r.at[r, q], self.p.partner())

    def cols(self, n):
        return pl.ds(n * self.half, self.half)

    def through(self, way, q):
        src = self.Y.at[self.p.cols[3], self.p.zs[q], self.p.c, :, self.cols(1 - way)]
        return self.copy(src, self.RH.at[way, q], self.h_s.at[way, q], self.h_r.at[way, q], self.p.side(way))

    def beside(self, way, q, n):
        r = 2 - way
        src = self.Y.at[self.p.cols[r], self.p.zs[q], self.p.c, :, self.cols(n)]
        dst = self.RX.at[way, q, :, self.cols(n)]
        return self.copy(src, dst, self.w_s.at[way, q, n], self.w_r.at[way, q, n], self.p.side(way))

    def to_z(self, k):
        src = self.Y.at[self.p.cols[0], self.p.zs[k], self.p.c]
        return self.copy(src, self.RZ.at[k - 1], self.rz_s.at[k - 1], self.rz_r.at[k - 1], self.p.zpeer(k))

    def first(self, q):
        p = self.p
        for r in (3, 1, 2, 0):
            self.pair(r, q).wait_recv()
            at = (p.cols[r], p.zs[q], p.c)
            self.Y[at] = (self.Y[at].astype(jnp.float32) + self.PR[r, q].astype(jnp.float32)).astype(jnp.bfloat16)
            if r == 3:
                self.through(0, q).start()
                self.through(1, q).start()
            if r == 1:
                self.beside(1, q, 1).start()
            if r == 2:
                self.beside(0, q, 0).start()

    def second(self, q):
        p = self.p
        for way in (1, 0):
            n = 1 - way
            self.through(way, q).wait_recv()
            at = (p.cols[2 - way], p.zs[q], p.c, slice(None), self.cols(n))
            self.Y[at] = (self.Y[at].astype(jnp.float32) + self.RH[way, q].astype(jnp.float32)).astype(jnp.bfloat16)
            self.beside(way, q, n).start()

    def third(self, q):
        p = self.p
        for way in (0, 1):
            for n in (0, 1):
                self.beside(way, q, n).wait_recv()
        if q:
            at = (p.cols[0], p.zs[q], p.c)
            total = self.Y[at].astype(jnp.float32) + self.RX[0, q].astype(jnp.float32) + self.RX[1, q].astype(jnp.float32)
            self.Y[at] = total.astype(jnp.bfloat16)
            self.to_z(q).start()

    def total(self):
        p = self.p
        for k in (1, 2, 3):
            self.to_z(k).wait_recv()
        at = (p.cols[0], p.zs[0], p.c)
        total = self.Y[at].astype(jnp.float32) + self.RX[0, 0].astype(jnp.float32) + self.RX[1, 0].astype(jnp.float32)
        for k in range(3):
            total = total + self.RZ[k].astype(jnp.float32)
        return total

    def finish(self):
        for k in (1, 2, 3):
            self.to_z(k).wait_send()
        for q in range(4):
            for way in (0, 1):
                self.through(way, q).wait_send()
                for n in (0, 1):
                    self.beside(way, q, n).wait_send()
            for r in range(4):
                self.pair(r, q).wait_send()


def dot(a, b):
    return jnp.dot(a, b, preferred_element_type=jnp.float32)


def dot_t(a, b):
    return lax.dot_general(a, b, (((1,), (1,)), ((), ())), preferred_element_type=jnp.float32)


def count(shape, dim):
    return lax.broadcasted_iota(jnp.int32, shape, dim).astype(jnp.float32)


def whole(values, n):
    return jnp.floor((values + 0.5) * (1.0 / n))


def ones(mask):
    return jnp.where(mask, 1.0, 0.0).astype(jnp.bfloat16)


class Slots:
    def __init__(self, tokens, experts, cap, pieces):
        self.tokens, self.experts, self.cap, self.pieces = tokens, experts, cap, pieces
        self.each = pieces * cap
        self.slots = experts * self.each

    def of_slots(self, v):
        e = whole(v, self.each)
        rest = v - e * self.each
        j = whole(rest, self.cap)
        return e, j, rest - j * self.cap

    def of_tokens(self, v):
        j = whole(v, self.tokens)
        return j, v - j * self.tokens

    def into(self, hit_t):
        n, q = self.slots, self.pieces * self.tokens
        before = dot(hit_t, ones(count((self.tokens, self.tokens), 0) < count((self.tokens, self.tokens), 1)))
        pick = ones(self.of_slots(count((n, self.experts), 0))[0] == count((n, self.experts), 1))
        wide = ones(count((self.tokens, q), 0) == self.of_tokens(count((self.tokens, q), 1))[1])
        hits = dot(dot(pick, hit_t).astype(jnp.bfloat16), wide)
        turn = dot(dot(pick, before.astype(jnp.bfloat16)).astype(jnp.bfloat16), wide)
        e, j, slot = self.of_slots(count((n, q), 0))
        jt = self.of_tokens(count((n, q), 1))[0]
        return ones((hits > 0.5) & (turn == slot) & (j == jt))

    def out_of(self, hit, hit_k):
        n, q = self.slots, self.pieces * self.tokens
        before = dot(ones(count((self.tokens, self.tokens), 1) < count((self.tokens, self.tokens), 0)), hit)
        pick = ones(self.of_slots(count((self.experts, n), 1))[0] == count((self.experts, n), 0))
        wide = ones(count((q, self.tokens), 1) == self.of_tokens(count((q, self.tokens), 0))[1])
        e, j, slot = self.of_slots(count((q, n), 1))
        jt = self.of_tokens(count((q, n), 0))[0]
        turn = dot(wide, dot(before.astype(jnp.bfloat16), pick).astype(jnp.bfloat16))
        place = (turn == slot) & (j == jt)
        return [ones((dot(wide, dot(one, pick).astype(jnp.bfloat16)) > 0.5) & place) for one in hit_k]

    def order(self, back):
        n = self.slots
        a, b = (count((n, n), 0), count((n, n), 1)) if not back else (count((n, n), 1), count((n, n), 0))
        j = whole(a, self.experts * self.cap)
        rest = a - j * (self.experts * self.cap)
        s = whole(rest, self.cap)
        return ones(b == s * self.each + j * self.cap + (rest - s * self.cap))


def kernel(
    sections, cap, pieces,
    stream_ref, ffn_gain_ref, router_ref, ids_ref, ids_t_ref, wg_ref, wu_ref, wd_ref, attn_gain_ref, wkv_ref,
    out_ref, kv_ref,
    X, Y, WG, WU, WD, H, PR, RX, RH, RZ, S, A, R, X2, K, local, d_s, d_r, b_s, b_r, k_s, k_r, *sems,
):
    p = Place()
    bf16, f32 = jnp.bfloat16, jnp.float32
    gather = Gather(p, X, sems[:8])
    reduce = Reduce(p, Y, PR, RX, RH, RZ, sems[8:16])
    gather2 = Gather(p, X2, sems[16:])
    tokens, model = stream_ref.shape
    rows = X.shape[-2]
    part = model // pieces
    cut = [slice(j * part, (j + 1) * part) for j in range(pieces)]
    slots = Slots(tokens, sections, cap, pieces)
    loads = [
        pltpu.make_async_copy(ref.at[0], buf, local.at[i])
        for i, (ref, buf) in enumerate(((wg_ref, WG), (wu_ref, WU), (wd_ref, WD)))
    ]
    for load in loads:
        load.start()

    def section(d):
        z = p.z if d % 2 == 0 else NZ - 1 - p.z
        return ((p.s + d) % sections, p.x * (NZ * 2) + z * 2 + p.c)

    m = lax.axis_index("mp")
    after = ((p.s + 1) % sections, m)
    ahead = ((p.s + sections - 1) % sections, m)
    far = (7, 1, 5, 3, 2, 6, 4)
    barrier = pltpu.get_barrier_semaphore()
    peers = p.peers() + [section(d) for d in far] + [after, ahead]
    for peer in peers:
        pl.semaphore_signal(barrier, inc=1, device_id=peer, device_id_type=MESH)

    def scaled(values, gain):
        return values * lax.rsqrt(jnp.mean(values * values, axis=-1, keepdims=True) + epsilon) * gain

    normed = scaled(stream_ref[...].astype(f32), ffn_gain_ref[...]).astype(bf16)
    e_of = lax.broadcasted_iota(jnp.int32, (sections, tokens), 0)
    hit_t = ones((e_of == ids_t_ref[0:1, :]) | (e_of == ids_t_ref[1:2, :]))
    stacked = jnp.concatenate([normed[:, c] for c in cut], axis=0)
    S[...] = dot(slots.into(hit_t), stacked).astype(bf16).reshape(S.shape)

    def give(src, dst, d, send, recv):
        return pltpu.make_async_remote_copy(
            src_ref=src.at[(p.s + d) % sections], dst_ref=dst.at[p.s], send_sem=send.at[d], recv_sem=recv.at[d],
            device_id=section(d), device_id_type=MESH,
        )

    pl.semaphore_wait(barrier, len(peers))
    for d in far:
        give(S, A, d, d_s, d_r).start()
    A[p.s] = S[p.s]
    logits = dot_t(normed, router_ref[...])
    t_of = lax.broadcasted_iota(jnp.int32, (tokens, sections), 1)
    named = [t_of == ids_ref[:, k:k + 1] for k in (0, 1)]
    chosen = [jnp.sum(jnp.where(one, logits, 0.0), axis=-1, keepdims=True) for one in named]
    share = 1.0 / (1.0 + jnp.exp(chosen[1] - chosen[0]))
    forth = slots.order(False)
    for d in far:
        give(S, A, d, d_s, d_r).wait_recv()
    block = dot(forth, A[...].reshape(slots.slots, part)).astype(bf16)
    own = (p.x, p.z, p.c)
    for j in range(pieces):
        X[p.x, p.z, p.c, :, cut[j]] = block[j * rows:(j + 1) * rows]

    gather.start()
    gather.spread_z(1)
    tile = min(512, model)
    order = ((0, 0), (1, 0), (2, 0), (0, 1), (3, 0), (1, 1), (2, 1), (3, 1))

    def before(i):
        if i == 0:
            gather.spread_x(0)
            for load in loads:
                load.wait()
        if i == 1:
            gather.spread_z(2)
            gather.spread_x(1)
        if i == 3:
            gather.spread_z(3)
        if i == 4:
            gather.spread_x2(0)
            gather.spread_x2(1)
            gather.spread_x(2)
        if i == 5:
            gather.spread_x(3)
        if i == 6:
            reduce.first(1)
        if i == 7:
            gather.spread_x2(2)
            gather.spread_x2(3)
            reduce.second(1)
        r, b = order[i]
        gather.need(r, (2 * b, 2 * b + 1))

    def behind(i):
        r, b = order[i]
        for q in (2 * b, 2 * b + 1):
            reduce.pair(r, q).start()

    def step(i, carry):
        for n in range(8):
            pl.when(i == n)(functools.partial(before, n))
        r = (i == 1) * 1 + (i == 2) * 2 + (i == 4) * 3 + (i == 5) * 1 + (i == 6) * 2 + (i == 7) * 3
        b = (i == 3) * 1 + (i >= 5) * 1
        shift = (r == 1) * 3 + (r == 2) * 1 + (r == 3) * 2
        col = (p.x + shift) % NX
        pair = (p.z // 2 + b) % 2
        zs = pl.ds(2 * pair, 2)
        value = X[col, zs].reshape(4 * rows, model)
        gate = dot_t(value, WG[...])
        up = dot_t(value, WU[...])
        H[...] = (gate / (1.0 + jnp.exp(-gate)) * up).astype(bf16)

        def down(n, carry):
            at = pl.ds(pl.multiple_of(n * tile, tile), tile)
            Y[col, zs, :, :, at] = dot(H[...], WD[:, at]).astype(bf16).reshape(2, 2, rows, tile)
            return carry

        lax.fori_loop(0, model // tile, down, 0)
        for n in range(8):
            pl.when(i == n)(functools.partial(behind, n))
        return carry

    lax.fori_loop(0, 8, step, 0)
    reduce.first(2)
    reduce.third(1)
    reduce.first(3)
    reduce.second(2)
    reduce.first(0)
    reduce.second(3)
    reduce.third(2)
    reduce.second(0)
    reduce.third(3)
    reduce.third(0)
    hit_k = [ones(one) for one in named]
    fetch = slots.out_of(ones(named[0] | named[1]), hit_k)
    sums = reduce.total().astype(bf16)
    for d in far:
        give(S, A, d, d_s, d_r).wait_send()
    packed = dot(slots.order(True), jnp.concatenate([sums[:, c] for c in cut], axis=0)).astype(bf16)
    S[...] = packed.reshape(S.shape)
    for d in far:
        give(S, R, d, b_s, b_r).start()
    R[p.s] = S[p.s]
    for d in far:
        give(S, R, d, b_s, b_r).wait_recv()
    back = R[...].reshape(slots.slots, part)
    share = jnp.concatenate([share] * pieces, axis=0)
    base = jnp.concatenate([stream_ref[:, c].astype(f32) for c in cut], axis=0)
    updated = (base + share * dot(fetch[0], back) + (1.0 - share) * dot(fetch[1], back)).astype(bf16)
    floats = updated.astype(f32)
    squares = jnp.sum(floats * floats, axis=-1, keepdims=True)
    total = squares[0:tokens]
    for j in range(1, pieces):
        total = total + squares[j * tokens:(j + 1) * tokens]
    scale = lax.rsqrt(total * (1.0 / model) + epsilon)
    for j in range(pieces):
        at = slice(j * tokens, (j + 1) * tokens)
        X2[p.x, p.z, p.c, :, cut[j]] = (floats[at] * scale * attn_gain_ref[:, cut[j]]).astype(bf16)
    gather2.start()
    for j in range(pieces):
        out_ref[:, cut[j]] = updated[j * tokens:(j + 1) * tokens]

    group = NZ * 2 * tokens

    def piece(r):
        at = pl.ds(pl.multiple_of(p.cols[r] * group, group), group)
        return pltpu.make_async_remote_copy(
            src_ref=K.at[p.cols[r]], dst_ref=kv_ref.at[:, at], send_sem=k_s.at[r], recv_sem=k_r.at[r],
            device_id=after, device_id_type=MESH,
        )

    def product(r):
        gather2.need(r, range(4))
        K[p.cols[r]] = dot_t(wkv_ref[...], X2[p.cols[r]].reshape(group, model)).astype(bf16)
        piece(r).start()

    gather2.spread_z(1)
    gather2.spread_x(0)
    gather2.spread_z(2)
    gather2.spread_x(1)
    gather2.spread_z(3)
    gather2.spread_x(2)
    gather2.spread_x2(0)
    product(0)
    gather2.spread_x(3)
    gather2.spread_x2(1)
    product(1)
    gather2.spread_x2(2)
    product(2)
    gather2.spread_x2(3)
    product(3)
    gather.finish()
    reduce.finish()
    gather2.finish()
    for d in far:
        give(S, R, d, b_s, b_r).wait_send()
    for r in range(4):
        piece(r).wait_recv()
    for r in range(4):
        piece(r).wait_send()


def body(stream, ffn_gain, router_weight, expert_ids, w_gate, w_up, w_down, attn_gain, w_kv):
    tokens, model = stream.shape
    sections = lax.axis_size("section")
    cap = min(tokens, 3 * tokens // router_weight.shape[1])
    pieces = 8
    rows = sections * cap
    hidden = w_gate.shape[-1]
    width = w_kv.shape[1]
    part = model // pieces
    bf16 = jnp.bfloat16
    dma = pltpu.SemaphoreType.DMA
    any_space = pl.BlockSpec(memory_space=pl.ANY)
    vmem = pl.BlockSpec(memory_space=pltpu.VMEM)
    exchange = pltpu.VMEM((sections, pieces * cap, part), bf16)
    stream_out, kv_t = pl.pallas_call(
        functools.partial(kernel, sections, cap, pieces),
        out_shape=(
            jax.ShapeDtypeStruct((tokens, model), bf16),
            jax.ShapeDtypeStruct((width, NX * NZ * 2 * tokens), bf16),
        ),
        in_specs=[vmem] * 5 + [any_space] * 3 + [vmem] * 2,
        out_specs=(vmem, vmem),
        scratch_shapes=[
            pltpu.VMEM((NX, NZ, 2, rows, model), bf16),
            pltpu.VMEM((NX, NZ, 2, rows, model), bf16),
            pltpu.VMEM((hidden, model), bf16),
            pltpu.VMEM((hidden, model), bf16),
            pltpu.VMEM((hidden, model), bf16),
            pltpu.VMEM((4 * rows, hidden), bf16),
            pltpu.VMEM((4, 4, rows, model), bf16),
            pltpu.VMEM((2, 4, rows, model), bf16),
            pltpu.VMEM((2, 4, rows, model // 2), bf16),
            pltpu.VMEM((3, rows, model), bf16),
            exchange,
            exchange,
            exchange,
            pltpu.VMEM((NX, NZ, 2, tokens, model), bf16),
            pltpu.VMEM((NX, width, NZ * 2 * tokens), bf16),
            dma((3,)),
            dma((8,)), dma((8,)), dma((8,)), dma((8,)),
            dma((4,)), dma((4,)),
            *Gather.sems(),
            *Reduce.sems(),
            *Gather.sems(),
        ],
        compiler_params=pltpu.CompilerParams(
            collective_id=0, has_side_effects=True, vmem_limit_bytes=VMEM_LIMIT
        ),
        name="layer",
    )(
        stream, ffn_gain[None, :], router_weight.T, expert_ids, expert_ids.T,
        jnp.swapaxes(w_gate, 1, 2), jnp.swapaxes(w_up, 1, 2), w_down, attn_gain[None, :], w_kv.T,
    )
    return (stream_out, kv_t.T)


def solution(mesh):
    in_specs = (
        P(("section", "mp"), None),
        P(),
        P(),
        P(("section", "mp"), None),
        P("section", None, "mp"),
        P("section", None, "mp"),
        P("section", "mp", None),
        P(),
        P(None, "mp"),
    )
    out_specs = (P(("section", "mp"), None), P("section", "mp"))
    return jax.shard_map(body, mesh=mesh, in_specs=in_specs, out_specs=out_specs, check_vma=False)
```

```python
import functools

import jax
import jax.numpy as jnp
from jax import lax
from jax.experimental import pallas as pl
from jax.experimental.pallas import tpu as pltpu
from jax.sharding import PartitionSpec as P

epsilon = 1e-05
MESH = pl.DeviceIdType.MESH
NX = 4
NZ = 4
VMEM_LIMIT = 66_000_000


class Place:
    def __init__(self):
        self.s = lax.axis_index("section")
        m = lax.axis_index("mp")
        self.x = m // (NZ * 2)
        self.z = (m // 2) % NZ
        self.c = m % 2
        z = self.z
        self.cols = [self.x, (self.x + 3) % NX, (self.x + 1) % NX, (self.x + 2) % NX]
        self.zs = [z, z + 1 - 2 * (z % 2), (z + 2) % NZ, NZ - 1 - z]

    def at(self, x, z, c):
        return (self.s, x * (NZ * 2) + z * 2 + c)

    def partner(self):
        return self.at(self.x, self.z, 1 - self.c)

    def side(self, way):
        return self.at(self.cols[2 - way], self.z, self.c)

    def zpeer(self, k):
        return self.at(self.x, self.zs[k], self.c)

    def peers(self):
        return [self.partner(), self.side(0), self.side(1)] + [self.zpeer(k) for k in (1, 2, 3)]


def mid_of(model):
    return model * 5 // 32


def half_of(way, half, mid):
    return pl.ds(way * (half + mid), half - mid)


class Gather:
    def __init__(self, place, X, sems):
        self.p, self.X = place, X
        self.zs_s, self.zs_r, self.xs_s, self.xs_r, self.x2_s, self.x2_r, self.p_s, self.p_r, self.m_s, self.m_r = sems
        self.half = X.shape[-1] // 2
        self.mid = mid_of(X.shape[-1])

    @staticmethod
    def sems():
        dma = pltpu.SemaphoreType.DMA
        return [
            dma((3,)), dma((3,)), dma((2, 4)), dma((2, 4)), dma((2, 4)), dma((2, 4)), dma((4, 4)), dma((4, 4)),
            dma((3,)), dma((3,)),
        ]

    def block(self, r, q, c):
        return self.X.at[self.p.cols[r], self.p.zs[q], c]

    def copy(self, ref, send, recv, to):
        return pltpu.make_async_remote_copy(
            src_ref=ref, dst_ref=ref, send_sem=send, recv_sem=recv, device_id=to, device_id_type=MESH
        )

    def to_z(self, k):
        return self.copy(self.block(0, 0, self.p.c), self.zs_s.at[k - 1], self.zs_r.at[k - 1], self.p.zpeer(k))

    def from_z(self, k):
        return self.copy(self.block(0, k, self.p.c), self.zs_s.at[k - 1], self.zs_r.at[k - 1], self.p.zpeer(k))

    def to_x(self, way, q):
        return self.copy(self.block(0, q, self.p.c), self.xs_s.at[way, q], self.xs_r.at[way, q], self.p.side(way))

    def from_x(self, way, q):
        return self.copy(self.block(1 + way, q, self.p.c), self.xs_s.at[way, q], self.xs_r.at[way, q], self.p.side(way))

    def part(self, r, q, way):
        return self.X.at[self.p.cols[r], self.p.zs[q], self.p.c, :, half_of(way, self.half, self.mid if q else 0)]

    def to_zmid(self, k):
        ref = self.X.at[self.p.cols[3], self.p.zs[0], self.p.c, :, pl.ds(self.half - self.mid, 2 * self.mid)]
        return self.copy(ref, self.m_s.at[k - 1], self.m_r.at[k - 1], self.p.zpeer(k))

    def from_zmid(self, k):
        ref = self.X.at[self.p.cols[3], self.p.zs[k], self.p.c, :, pl.ds(self.half - self.mid, 2 * self.mid)]
        return self.copy(ref, self.m_s.at[k - 1], self.m_r.at[k - 1], self.p.zpeer(k))

    def on_x(self, way, q):
        return self.copy(self.part(1 + way, q, way), self.x2_s.at[way, q], self.x2_r.at[way, q], self.p.side(way))

    def from_x2(self, way, q):
        return self.copy(self.part(3, q, way), self.x2_s.at[way, q], self.x2_r.at[way, q], self.p.side(way))

    def pair(self, r, q):
        return self.copy(self.block(r, q, self.p.c), self.p_s.at[r, q], self.p_r.at[r, q], self.p.partner())

    def from_pair(self, r, q):
        return self.copy(self.block(r, q, 1 - self.p.c), self.p_s.at[r, q], self.p_r.at[r, q], self.p.partner())

    def start(self):
        self.to_x(0, 0).start()
        self.to_x(1, 0).start()
        for k in (1, 2, 3):
            self.to_z(k).start()
        self.pair(0, 0).start()

    def spread_z(self, k):
        self.from_z(k).wait_recv()
        self.to_x(0, k).start()
        self.to_x(1, k).start()
        self.pair(0, k).start()

    def spread_x(self, q):
        for way in (0, 1):
            self.from_x(way, q).wait_recv()
            self.on_x(way, q).start()
        for way in (0, 1):
            self.pair(1 + way, q).start()

    def spread_x2(self, q):
        for way in (0, 1):
            self.from_x2(way, q).wait_recv()
        if q:
            self.from_zmid(q).wait_recv()
        else:
            for k in (1, 2, 3):
                self.to_zmid(k).start()
        self.pair(3, q).start()

    def need(self, r, qs):
        for q in qs:
            self.from_pair(r, q).wait_recv()

    def finish(self):
        for k in (1, 2, 3):
            self.to_z(k).wait_send()
            self.to_zmid(k).wait_send()
        for q in range(4):
            for way in (0, 1):
                self.to_x(way, q).wait_send()
                self.on_x(way, q).wait_send()
            for r in range(4):
                self.pair(r, q).wait_send()


def enter(peers):
    barrier = pltpu.get_barrier_semaphore()
    for peer in peers:
        pl.semaphore_signal(barrier, inc=1, device_id=peer, device_id_type=MESH)
    pl.semaphore_wait(barrier, len(peers))


class Reduce:
    def __init__(self, place, Y, PR, RX, RH, RZ, RM, sems):
        self.p, self.Y, self.PR, self.RX, self.RH, self.RZ, self.RM = place, Y, PR, RX, RH, RZ, RM
        self.py_s, self.py_r, self.h_s, self.h_r, self.w_s, self.w_r, self.rz_s, self.rz_r, self.m_s, self.m_r = sems
        self.half = Y.shape[-1] // 2
        self.mid = mid_of(Y.shape[-1])

    @staticmethod
    def sems():
        dma = pltpu.SemaphoreType.DMA
        return [
            dma((4, 4)), dma((4, 4)), dma((2, 4)), dma((2, 4)), dma((2, 4, 2)), dma((2, 4, 2)), dma((3,)), dma((3,)),
            dma((3,)), dma((3,)),
        ]

    def copy(self, src, dst, send, recv, to):
        return pltpu.make_async_remote_copy(
            src_ref=src, dst_ref=dst, send_sem=send, recv_sem=recv, device_id=to, device_id_type=MESH
        )

    def pair(self, r, q):
        src = self.Y.at[self.p.cols[r], self.p.zs[q], 1 - self.p.c]
        return self.copy(src, self.PR.at[r, q], self.py_s.at[r, q], self.py_r.at[r, q], self.p.partner())

    def cols(self, n):
        return pl.ds(n * self.half, self.half)

    def through(self, way, q):
        at = half_of(1 - way, self.half, self.mid if q else 0)
        src = self.Y.at[self.p.cols[3], self.p.zs[q], self.p.c, :, at]
        dst = self.RH.at[q, :, at]
        return self.copy(src, dst, self.h_s.at[way, q], self.h_r.at[way, q], self.p.side(way))

    def middle(self):
        return pl.ds(self.half - self.mid, 2 * self.mid)

    def to_zmid(self, k):
        src = self.Y.at[self.p.cols[3], self.p.zs[k], self.p.c, :, self.middle()]
        return self.copy(src, self.RM.at[k - 1], self.m_s.at[k - 1], self.m_r.at[k - 1], self.p.zpeer(k))

    def beside(self, way, q, n):
        r = 2 - way
        src = self.Y.at[self.p.cols[r], self.p.zs[q], self.p.c, :, self.cols(n)]
        dst = self.RX.at[way, q, :, self.cols(n)]
        return self.copy(src, dst, self.w_s.at[way, q, n], self.w_r.at[way, q, n], self.p.side(way))

    def to_z(self, k):
        src = self.Y.at[self.p.cols[0], self.p.zs[k], self.p.c]
        return self.copy(src, self.RZ.at[k - 1], self.rz_s.at[k - 1], self.rz_r.at[k - 1], self.p.zpeer(k))

    def first(self, q):
        p = self.p
        for r in (3, 1, 2, 0):
            self.pair(r, q).wait_recv()
            at = (p.cols[r], p.zs[q], p.c)
            self.Y[at] = (self.Y[at].astype(jnp.float32) + self.PR[r, q].astype(jnp.float32)).astype(jnp.bfloat16)
            if r == 3:
                if q:
                    self.to_zmid(q).start()
                else:
                    for k in (1, 2, 3):
                        self.to_zmid(k).wait_recv()
                    mid = (p.cols[r], p.zs[q], p.c, slice(None), self.middle())
                    total = self.Y[mid].astype(jnp.float32)
                    for k in range(3):
                        total = total + self.RM[k].astype(jnp.float32)
                    self.Y[mid] = total.astype(jnp.bfloat16)
                self.through(0, q).start()
                self.through(1, q).start()
            if r == 1:
                self.beside(1, q, 1).start()
            if r == 2:
                self.beside(0, q, 0).start()

    def second(self, q):
        p = self.p
        for way in (1, 0):
            n = 1 - way
            self.through(way, q).wait_recv()
            part = half_of(n, self.half, self.mid if q else 0)
            at = (p.cols[2 - way], p.zs[q], p.c, slice(None), part)
            self.Y[at] = (self.Y[at].astype(jnp.float32) + self.RH[q, :, part].astype(jnp.float32)).astype(jnp.bfloat16)
            self.beside(way, q, n).start()

    def third(self, q):
        p = self.p
        for way in (0, 1):
            for n in (0, 1):
                self.beside(way, q, n).wait_recv()
        if q:
            at = (p.cols[0], p.zs[q], p.c)
            total = self.Y[at].astype(jnp.float32) + self.RX[0, q].astype(jnp.float32) + self.RX[1, q].astype(jnp.float32)
            self.Y[at] = total.astype(jnp.bfloat16)
            self.to_z(q).start()

    def total(self):
        p = self.p
        for k in (1, 2, 3):
            self.to_z(k).wait_recv()
        at = (p.cols[0], p.zs[0], p.c)
        total = self.Y[at].astype(jnp.float32) + self.RX[0, 0].astype(jnp.float32) + self.RX[1, 0].astype(jnp.float32)
        for k in range(3):
            total = total + self.RZ[k].astype(jnp.float32)
        return total

    def finish(self):
        for k in (1, 2, 3):
            self.to_z(k).wait_send()
            self.to_zmid(k).wait_send()
        for q in range(4):
            for way in (0, 1):
                self.through(way, q).wait_send()
                for n in (0, 1):
                    self.beside(way, q, n).wait_send()
            for r in range(4):
                self.pair(r, q).wait_send()


def dot(a, b):
    return jnp.dot(a, b, preferred_element_type=jnp.float32)


def dot_t(a, b):
    return lax.dot_general(a, b, (((1,), (1,)), ((), ())), preferred_element_type=jnp.float32)


def count(shape, dim):
    return lax.broadcasted_iota(jnp.int32, shape, dim).astype(jnp.float32)


def whole(values, n):
    return jnp.floor((values + 0.5) * (1.0 / n))


def ones(mask):
    return jnp.where(mask, 1.0, 0.0).astype(jnp.bfloat16)


class Slots:
    def __init__(self, tokens, experts, cap, pieces):
        self.tokens, self.experts, self.cap, self.pieces = tokens, experts, cap, pieces
        self.each = pieces * cap
        self.slots = experts * self.each

    def of_slots(self, v):
        e = whole(v, self.each)
        rest = v - e * self.each
        j = whole(rest, self.cap)
        return e, j, rest - j * self.cap

    def of_tokens(self, v):
        j = whole(v, self.tokens)
        return j, v - j * self.tokens

    def into(self, hit_t):
        n, q = self.slots, self.pieces * self.tokens
        before = dot(hit_t, ones(count((self.tokens, self.tokens), 0) < count((self.tokens, self.tokens), 1)))
        pick = ones(self.of_slots(count((n, self.experts), 0))[0] == count((n, self.experts), 1))
        wide = ones(count((self.tokens, q), 0) == self.of_tokens(count((self.tokens, q), 1))[1])
        hits = dot(dot(pick, hit_t).astype(jnp.bfloat16), wide)
        turn = dot(dot(pick, before.astype(jnp.bfloat16)).astype(jnp.bfloat16), wide)
        e, j, slot = self.of_slots(count((n, q), 0))
        jt = self.of_tokens(count((n, q), 1))[0]
        return ones((hits > 0.5) & (turn == slot) & (j == jt))

    def out_of(self, hit, hit_k):
        n, q = self.slots, self.pieces * self.tokens
        before = dot(ones(count((self.tokens, self.tokens), 1) < count((self.tokens, self.tokens), 0)), hit)
        pick = ones(self.of_slots(count((self.experts, n), 1))[0] == count((self.experts, n), 0))
        wide = ones(count((q, self.tokens), 1) == self.of_tokens(count((q, self.tokens), 0))[1])
        e, j, slot = self.of_slots(count((q, n), 1))
        jt = self.of_tokens(count((q, n), 0))[0]
        turn = dot(wide, dot(before.astype(jnp.bfloat16), pick).astype(jnp.bfloat16))
        place = (turn == slot) & (j == jt)
        return [ones((dot(wide, dot(one, pick).astype(jnp.bfloat16)) > 0.5) & place) for one in hit_k]

    def order(self, back):
        n = self.slots
        a, b = (count((n, n), 0), count((n, n), 1)) if not back else (count((n, n), 1), count((n, n), 0))
        j = whole(a, self.experts * self.cap)
        rest = a - j * (self.experts * self.cap)
        s = whole(rest, self.cap)
        return ones(b == s * self.each + j * self.cap + (rest - s * self.cap))


def kernel(
    sections, cap, pieces,
    stream_ref, ffn_gain_ref, router_ref, ids_t_ref, wg_ref, wu_ref, wd_ref, attn_gain_ref, wkv_ref,
    out_ref, kv_ref,
    X, Y, WG, WU, WD, H, PR, RX, RH, RZ, RM, S, A, R, X2, WK, K, KR,
    local, d_s, d_r, b_s, b_r, k_s, k_r, wz_s, wz_r, wy_s, wy_r, n_s, n_r, n2_s, n2_r, np_s, np_r, *sems,
):
    p = Place()
    bf16, f32 = jnp.bfloat16, jnp.float32
    gather = Gather(p, X, sems[:10])
    reduce = Reduce(p, Y, PR, RX, RH, RZ, RM, sems[10:])
    tokens, model = stream_ref.shape
    rows = X.shape[-2]
    part = model // pieces
    cut = [slice(j * part, (j + 1) * part) for j in range(pieces)]
    slots = Slots(tokens, sections, cap, pieces)
    loads = [
        pltpu.make_async_copy(ref.at[0], buf, local.at[i])
        for i, (ref, buf) in enumerate(((wg_ref, WG), (wu_ref, WU), (wd_ref, WD)))
    ]
    for load in loads:
        load.start()
    own_wkv = pltpu.make_async_copy(wkv_ref, WK.at[p.z], local.at[3])
    own_wkv.start()

    def section(d):
        z = p.z if d % 2 == 0 else NZ - 1 - p.z
        return ((p.s + d) % sections, p.x * (NZ * 2) + z * 2 + p.c)

    def next_at(k, d):
        return ((p.s + d) % sections, p.x * (NZ * 2) + p.zs[k] * 2 + p.c)

    far = (7, 1, 5, 3, 2, 6, 4)
    barrier = pltpu.get_barrier_semaphore()
    peers = p.peers() + [section(d) for d in far]
    peers = peers + [next_at(k, d) for k in (0, 1, 2) for d in (1, sections - 1)]
    for peer in peers:
        pl.semaphore_signal(barrier, inc=1, device_id=peer, device_id_type=MESH)

    def scaled(values, gain):
        return values * lax.rsqrt(jnp.mean(values * values, axis=-1, keepdims=True) + epsilon) * gain

    normed = scaled(stream_ref[...].astype(f32), ffn_gain_ref[...]).astype(bf16)
    e_of = lax.broadcasted_iota(jnp.int32, (sections, tokens), 0)
    hit_t = ones((e_of == ids_t_ref[0:1, :]) | (e_of == ids_t_ref[1:2, :]))
    stacked = jnp.concatenate([normed[:, c] for c in cut], axis=0)
    S[...] = dot(slots.into(hit_t), stacked).astype(bf16).reshape(S.shape)

    def give(src, dst, d, send, recv):
        return pltpu.make_async_remote_copy(
            src_ref=src.at[(p.s + d) % sections], dst_ref=dst.at[p.s], send_sem=send.at[d], recv_sem=recv.at[d],
            device_id=section(d), device_id_type=MESH,
        )

    pl.semaphore_wait(barrier, len(peers))
    for d in far:
        give(S, A, d, d_s, d_r).start()
    A[p.s] = S[p.s]
    logits = dot_t(normed, router_ref[...])
    same = ones(count((tokens, tokens), 0) == count((tokens, tokens), 1))
    named = [dot_t(same, ones(e_of == ids_t_ref[k:k + 1, :])) > 0.5 for k in (0, 1)]
    chosen = [jnp.sum(jnp.where(one, logits, 0.0), axis=-1, keepdims=True) for one in named]
    share = 1.0 / (1.0 + jnp.exp(chosen[1] - chosen[0]))
    forth = slots.order(False)
    for d in far:
        give(S, A, d, d_s, d_r).wait_recv()
    block = dot(forth, A[...].reshape(slots.slots, part)).astype(bf16)
    own = (p.x, p.z, p.c)
    for j in range(pieces):
        X[p.x, p.z, p.c, :, cut[j]] = block[j * rows:(j + 1) * rows]

    gather.start()
    gather.spread_z(1)
    tile = min(512, model)

    y = p.s // 2
    quarter = model // 4

    def wkv_copy(z, y, send, recv, to):
        ref = WK.at[z, :, pl.ds(pl.multiple_of(y * quarter, quarter), quarter)]
        return pltpu.make_async_remote_copy(
            src_ref=ref, dst_ref=ref, send_sem=send, recv_sem=recv, device_id=to, device_id_type=MESH
        )

    def wkv_z(k, of):
        return wkv_copy(p.zs[of], y, wz_s.at[k - 1], wz_r.at[k - 1], p.zpeer(k))

    def wkv_y(k, d, of):
        return wkv_copy(p.zs[k], (y + of) % 4, wy_s.at[k - 1, d - 1], wy_r.at[k - 1, d - 1], section(2 * d))

    order = ((0, 0), (1, 0), (2, 0), (0, 1), (3, 0), (1, 1), (2, 1), (3, 1))

    def before(i):
        if i == 0:
            gather.spread_x(0)
            for load in loads:
                load.wait()
        if i == 1:
            gather.spread_x(1)
            gather.spread_z(2)
        if i == 3:
            gather.spread_z(3)
        if i == 4:
            gather.spread_x2(0)
            gather.spread_x2(1)
            gather.spread_x(2)
        if i == 5:
            gather.spread_x(3)
            own_wkv.wait()
            for k in (1, 2, 3):
                wkv_z(k, 0).start()
        if i == 6:
            reduce.first(1)
        if i == 7:
            gather.spread_x2(2)
            gather.spread_x2(3)
            reduce.second(1)
        r, b = order[i]
        gather.need(r, (2 * b, 2 * b + 1))

    def behind(i):
        r, b = order[i]
        for q in (2 * b, 2 * b + 1):
            reduce.pair(r, q).start()

    def step(i, carry):
        for n in range(8):
            pl.when(i == n)(functools.partial(before, n))
        r = (i == 1) * 1 + (i == 2) * 2 + (i == 4) * 3 + (i == 5) * 1 + (i == 6) * 2 + (i == 7) * 3
        b = (i == 3) * 1 + (i >= 5) * 1
        shift = (r == 1) * 3 + (r == 2) * 1 + (r == 3) * 2
        col = (p.x + shift) % NX
        pair = (p.z // 2 + b) % 2
        zs = pl.ds(2 * pair, 2)
        value = X[col, zs].reshape(4 * rows, model)
        gate = dot_t(value, WG[...])
        up = dot_t(value, WU[...])
        H[...] = (gate / (1.0 + jnp.exp(-gate)) * up).astype(bf16)

        def down(n, carry):
            at = pl.ds(pl.multiple_of(n * tile, tile), tile)
            Y[col, zs, :, :, at] = dot(H[...], WD[:, at]).astype(bf16).reshape(2, 2, rows, tile)
            return carry

        lax.fori_loop(0, model // tile, down, 0)
        for n in range(8):
            pl.when(i == n)(functools.partial(behind, n))
        return carry

    lax.fori_loop(0, 8, step, 0)
    reduce.first(2)
    reduce.third(1)
    reduce.first(3)
    reduce.second(2)
    reduce.first(0)
    for k in (1, 2, 3):
        wkv_z(k, k).wait_recv()
        for d in (1, 2, 3):
            wkv_y(k, d, 0).start()
    reduce.second(3)
    reduce.third(2)
    reduce.second(0)
    reduce.third(3)
    reduce.third(0)
    hit_k = [ones(one) for one in named]
    fetch = slots.out_of(ones(named[0] | named[1]), hit_k)
    sums = reduce.total().astype(bf16)
    for d in far:
        give(S, A, d, d_s, d_r).wait_send()
    packed = dot(slots.order(True), jnp.concatenate([sums[:, c] for c in cut], axis=0)).astype(bf16)
    S[...] = packed.reshape(S.shape)
    for d in far:
        give(S, R, d, b_s, b_r).start()
    R[p.s] = S[p.s]
    for d in far:
        give(S, R, d, b_s, b_r).wait_recv()
    back = R[...].reshape(slots.slots, part)
    share = jnp.concatenate([share] * pieces, axis=0)
    base = jnp.concatenate([stream_ref[:, c].astype(f32) for c in cut], axis=0)
    updated = (base + share * dot(fetch[0], back) + (1.0 - share) * dot(fetch[1], back)).astype(bf16)
    floats = updated.astype(f32)
    squares = jnp.sum(floats * floats, axis=-1, keepdims=True)
    total = squares[0:tokens]
    for j in range(1, pieces):
        total = total + squares[j * tokens:(j + 1) * tokens]
    scale = lax.rsqrt(total * (1.0 / model) + epsilon)
    for j in range(pieces):
        at = slice(j * tokens, (j + 1) * tokens)
        X2[p.x, p.c, :, cut[j]] = (floats[at] * scale * attn_gain_ref[:, cut[j]]).astype(bf16)

    half = model // 2

    def row(c, r, at, send, recv, to):
        ref = X2.at[p.cols[r], c, :, at]
        return pltpu.make_async_remote_copy(
            src_ref=ref, dst_ref=ref, send_sem=send, recv_sem=recv, device_id=to, device_id_type=MESH
        )

    every = pl.ds(0, model)

    def row_x(way, r):
        return row(p.c, r, every, n_s.at[way], n_r.at[way], p.side(way))

    def row_x2(way, r):
        return row(p.c, r, pl.ds(way * half, half), n2_s.at[way], n2_r.at[way], p.side(way))

    def row_pair(r, c):
        return row(c, r, every, np_s.at[r], np_r.at[r], p.partner())

    for way in (0, 1):
        row_x(way, 0).start()
    row_pair(0, p.c).start()
    for j in range(pieces):
        out_ref[:, cut[j]] = updated[j * tokens:(j + 1) * tokens]
    for way in (0, 1):
        row_x(way, 1 + way).wait_recv()
        row_x2(way, 1 + way).start()
    for way in (0, 1):
        row_pair(1 + way, p.c).start()
    for k in (1, 2, 3):
        for d in (1, 2, 3):
            wkv_y(k, d, 4 - d).wait_recv()
    for way in (0, 1):
        row_x2(way, 3).wait_recv()
    row_pair(3, p.c).start()
    for r in range(4):
        row_pair(r, 1 - p.c).wait_recv()
    width = WK.shape[1]
    each = NX * 2 * tokens
    K[...] = dot_t(WK[...].reshape(NZ * width, model), X2[...].reshape(each, model)).astype(bf16).reshape(K.shape)

    def piece(k):
        return pltpu.make_async_remote_copy(
            src_ref=K.at[p.zs[k]], dst_ref=KR.at[p.z], send_sem=k_s.at[k], recv_sem=k_r.at[k],
            device_id=next_at(k, 1), device_id_type=MESH,
        )

    for k in (3, 1, 2, 0):
        piece(k).start()
    a, b = count((NZ * each, NZ * each), 0), count((NZ * each, NZ * each), 1)
    z_of = whole(a, each)
    x_of = whole(a - z_of * each, 2 * tokens)
    t_of = a - z_of * each - x_of * (2 * tokens)
    into = ones(b == x_of * each + z_of * (2 * tokens) + t_of)
    for k in range(4):
        piece(k).wait_recv()
    kv_ref[...] = dot(jnp.concatenate([KR[z] for z in range(NZ)], axis=1), into).astype(bf16)
    gather.finish()
    reduce.finish()
    for k in (1, 2, 3):
        wkv_z(k, 0).wait_send()
        for d in (1, 2, 3):
            wkv_y(k, d, 0).wait_send()
    for d in far:
        give(S, R, d, b_s, b_r).wait_send()
    for way in (0, 1):
        row_x(way, 0).wait_send()
        row_x2(way, 1 + way).wait_send()
    for r in range(4):
        row_pair(r, p.c).wait_send()
        piece(r).wait_send()


def body(stream, ffn_gain, router_weight, expert_ids, w_gate, w_up, w_down, attn_gain, w_kv):
    tokens, model = stream.shape
    sections = lax.axis_size("section")
    cap = min(tokens, 3 * tokens // router_weight.shape[1])
    pieces = 8
    rows = sections * cap
    hidden = w_gate.shape[-1]
    width = w_kv.shape[1]
    part = model // pieces
    bf16 = jnp.bfloat16
    dma = pltpu.SemaphoreType.DMA
    any_space = pl.BlockSpec(memory_space=pl.ANY)
    vmem = pl.BlockSpec(memory_space=pltpu.VMEM)
    exchange = pltpu.VMEM((sections, pieces * cap, part), bf16)
    stream_out, kv_t = pl.pallas_call(
        functools.partial(kernel, sections, cap, pieces),
        out_shape=(
            jax.ShapeDtypeStruct((tokens, model), bf16),
            jax.ShapeDtypeStruct((width, NX * NZ * 2 * tokens), bf16),
        ),
        in_specs=[vmem] * 4 + [any_space] * 3 + [vmem, any_space],
        out_specs=(vmem, vmem),
        scratch_shapes=[
            pltpu.VMEM((NX, NZ, 2, rows, model), bf16),
            pltpu.VMEM((NX, NZ, 2, rows, model), bf16),
            pltpu.VMEM((hidden, model), bf16),
            pltpu.VMEM((hidden, model), bf16),
            pltpu.VMEM((hidden, model), bf16),
            pltpu.VMEM((4 * rows, hidden), bf16),
            pltpu.VMEM((4, 4, rows, model), bf16),
            pltpu.VMEM((2, 4, rows, model), bf16),
            pltpu.VMEM((4, rows, model), bf16),
            pltpu.VMEM((3, rows, model), bf16),
            pltpu.VMEM((3, rows, 2 * mid_of(model)), bf16),
            exchange,
            exchange,
            exchange,
            pltpu.VMEM((NX, 2, tokens, model), bf16),
            pltpu.VMEM((NZ, width, model), bf16),
            pltpu.VMEM((NZ, width, NX * 2 * tokens), bf16),
            pltpu.VMEM((NZ, width, NX * 2 * tokens), bf16),
            dma((4,)),
            dma((8,)), dma((8,)), dma((8,)), dma((8,)),
            dma((4,)), dma((4,)),
            dma((3,)), dma((3,)), dma((3, 3)), dma((3, 3)),
            dma((2,)), dma((2,)), dma((2,)), dma((2,)), dma((4,)), dma((4,)),
            *Gather.sems(),
            *Reduce.sems(),
        ],
        compiler_params=pltpu.CompilerParams(
            collective_id=0, has_side_effects=True, vmem_limit_bytes=VMEM_LIMIT
        ),
        name="layer",
    )(
        stream, ffn_gain[None, :], router_weight.T, expert_ids.T,
        jnp.swapaxes(w_gate, 1, 2), jnp.swapaxes(w_up, 1, 2), w_down, attn_gain[None, :], w_kv.T,
    )
    return (stream_out, kv_t.T)


def solution(mesh):
    in_specs = (
        P(("section", "mp"), None),
        P(),
        P(),
        P(("section", "mp"), None),
        P("section", None, "mp"),
        P("section", None, "mp"),
        P("section", "mp", None),
        P(),
        P(None, "mp"),
    )
    out_specs = (P(("section", "mp"), None), P("section", "mp"))
    return jax.shard_map(body, mesh=mesh, in_specs=in_specs, out_specs=out_specs, check_vma=False)
```

```python
import functools

import jax
import jax.numpy as jnp
from jax import lax
from jax.experimental import pallas as pl
from jax.experimental.pallas import tpu as pltpu
from jax.sharding import PartitionSpec as P

epsilon = 1e-05
MESH = pl.DeviceIdType.MESH
NX = 4
NZ = 4
VMEM_LIMIT = 66_000_000


class Place:
    def __init__(self):
        self.s = lax.axis_index("section")
        m = lax.axis_index("mp")
        self.x = m // (NZ * 2)
        self.z = (m // 2) % NZ
        self.c = m % 2
        z = self.z
        self.cols = [self.x, (self.x + 3) % NX, (self.x + 1) % NX, (self.x + 2) % NX]
        self.zs = [z, z + 1 - 2 * (z % 2), (z + 2) % NZ, NZ - 1 - z]
        self.inner = (z == 1) | (z == 2)
        self.zq = [z, z + 1 - 2 * (z % 2), 2 - z // 2, 3 - 3 * (z // 2)]

    def at(self, x, z, c):
        return (self.s, x * (NZ * 2) + z * 2 + c)

    def partner(self):
        return self.at(self.x, self.z, 1 - self.c)

    def side(self, way):
        return self.at(self.cols[2 - way], self.z, self.c)

    def zpeer(self, k):
        return self.at(self.x, self.zs[k], self.c)

    def peers(self):
        return [self.partner(), self.side(0), self.side(1)] + [self.zpeer(k) for k in (1, 2, 3)]


def mid_of(model):
    return model * 5 // 32


def far_of(model):
    return model // 4


def half_of(way, half, mid):
    return pl.ds(way * (half + mid), half - mid)


class Gather:
    def __init__(self, place, X, sems):
        self.p, self.X = place, X
        self.zo_s, self.zf_s, self.zs_r, self.xs_s, self.xs_r, self.x2_s, self.x2_r, self.p_s, self.p_r, self.m_s, self.m_r = sems
        self.half = X.shape[-1] // 2
        self.mid = far_of(X.shape[-1])

    @staticmethod
    def sems():
        dma = pltpu.SemaphoreType.DMA
        return [
            dma((2,)), dma((3,)), dma((3,)), dma((2, 4)), dma((2, 4)), dma((2, 4)), dma((2, 4)), dma((4, 4)), dma((4, 4)),
            dma((3,)), dma((3,)),
        ]

    def block(self, r, q, c):
        return self.X.at[self.p.cols[r], self.p.zq[q], c]

    def copy(self, ref, send, recv, to):
        return pltpu.make_async_remote_copy(
            src_ref=ref, dst_ref=ref, send_sem=send, recv_sem=recv, device_id=to, device_id_type=MESH
        )

    def own_z(self, n):
        return self.copy(self.block(0, 0, self.p.c), self.zo_s.at[n], self.zs_r.at[n], self.p.at(self.p.x, self.p.zq[1 + n], self.p.c))

    def on_z(self, q):
        to, kind = (2, 3) if q == 1 else (1, q)
        return self.copy(self.block(0, q, self.p.c), self.zf_s.at[q - 1], self.zs_r.at[kind - 1], self.p.at(self.p.x, self.p.zq[to], self.p.c))

    def from_z(self, q):
        return self.copy(self.block(0, q, self.p.c), self.zf_s.at[q - 1], self.zs_r.at[q - 1], self.p.partner())

    def to_x(self, way, q):
        return self.copy(self.block(0, q, self.p.c), self.xs_s.at[way, q], self.xs_r.at[way, q], self.p.side(way))

    def from_x(self, way, q):
        return self.copy(self.block(1 + way, q, self.p.c), self.xs_s.at[way, q], self.xs_r.at[way, q], self.p.side(way))

    def part(self, r, q, way):
        return self.X.at[self.p.cols[r], self.p.zq[q], self.p.c, :, half_of(way, self.half, self.mid if q else 0)]

    def to_zmid(self, k):
        ref = self.X.at[self.p.cols[3], self.p.zs[0], self.p.c, :, pl.ds(self.half - self.mid, 2 * self.mid)]
        return self.copy(ref, self.m_s.at[k - 1], self.m_r.at[k - 1], self.p.zpeer(k))

    def from_zmid(self, k):
        ref = self.X.at[self.p.cols[3], self.p.zs[k], self.p.c, :, pl.ds(self.half - self.mid, 2 * self.mid)]
        return self.copy(ref, self.m_s.at[k - 1], self.m_r.at[k - 1], self.p.zpeer(k))

    def on_x(self, way, q):
        return self.copy(self.part(1 + way, q, way), self.x2_s.at[way, q], self.x2_r.at[way, q], self.p.side(way))

    def from_x2(self, way, q):
        return self.copy(self.part(3, q, way), self.x2_s.at[way, q], self.x2_r.at[way, q], self.p.side(way))

    def pair(self, r, q):
        return self.copy(self.block(r, q, self.p.c), self.p_s.at[r, q], self.p_r.at[r, q], self.p.partner())

    def from_pair(self, r, q):
        return self.copy(self.block(r, q, 1 - self.p.c), self.p_s.at[r, q], self.p_r.at[r, q], self.p.partner())

    def start(self):
        self.to_x(0, 0).start()
        self.to_x(1, 0).start()
        self.own_z(0).start()
        pl.when(self.p.inner)(lambda: self.own_z(1).start())
        self.pair(0, 0).start()

    def spread_z(self, k):
        self.from_z(k).wait_recv()
        pl.when(self.p.inner)(lambda: self.on_z(k).start())
        self.to_x(0, k).start()
        self.to_x(1, k).start()
        self.pair(0, k).start()

    def spread_x(self, q):
        for way in (0, 1):
            self.from_x(way, q).wait_recv()
            self.on_x(way, q).start()
        for way in (0, 1):
            self.pair(1 + way, q).start()

    def spread_x2(self, q):
        for way in (0, 1):
            self.from_x2(way, q).wait_recv()
        if q == 0:
            for k in (1, 2, 3):
                self.to_zmid(k).start()
        if q == 1:
            self.from_zmid(1).wait_recv()
        if q < 2:
            self.pair(3, q).start()
        if q == 3:
            for k in (2, 3):
                self.from_zmid(k).wait_recv()
            for k in (2, 3):
                self.pair(3, k).start()

    def need(self, r, qs):
        for q in qs:
            self.from_pair(r, q).wait_recv()

    def finish(self):
        self.own_z(0).wait_send()

        def inner():
            self.own_z(1).wait_send()
            for q in (1, 2, 3):
                self.on_z(q).wait_send()

        pl.when(self.p.inner)(inner)
        for k in (1, 2, 3):
            self.to_zmid(k).wait_send()
        for q in range(4):
            for way in (0, 1):
                self.to_x(way, q).wait_send()
                self.on_x(way, q).wait_send()
            for r in range(4):
                self.pair(r, q).wait_send()


def enter(peers):
    barrier = pltpu.get_barrier_semaphore()
    for peer in peers:
        pl.semaphore_signal(barrier, inc=1, device_id=peer, device_id_type=MESH)
    pl.semaphore_wait(barrier, len(peers))


class Reduce:
    def __init__(self, place, Y, PR, RX, RH, RZ, RM, sems):
        self.p, self.Y, self.PR, self.RX, self.RH, self.RZ, self.RM = place, Y, PR, RX, RH, RZ, RM
        self.py_s, self.py_r, self.h_s, self.h_r, self.w_s, self.w_r, self.rz_s, self.rz_r, self.m_s, self.m_r = sems
        self.half = Y.shape[-1] // 2
        self.mid = mid_of(Y.shape[-1])

    @staticmethod
    def sems():
        dma = pltpu.SemaphoreType.DMA
        return [
            dma((4, 4)), dma((4, 4)), dma((2, 4)), dma((2, 4)), dma((2, 4, 2)), dma((2, 4, 2)), dma((3,)), dma((3,)),
            dma((3,)), dma((3,)),
        ]

    def copy(self, src, dst, send, recv, to):
        return pltpu.make_async_remote_copy(
            src_ref=src, dst_ref=dst, send_sem=send, recv_sem=recv, device_id=to, device_id_type=MESH
        )

    def pair(self, r, q):
        src = self.Y.at[self.p.cols[r], self.p.zs[q], 1 - self.p.c]
        return self.copy(src, self.PR.at[r, q], self.py_s.at[r, q], self.py_r.at[r, q], self.p.partner())

    def cols(self, n):
        return pl.ds(n * self.half, self.half)

    def through(self, way, q):
        at = half_of(1 - way, self.half, self.mid if q else 0)
        src = self.Y.at[self.p.cols[3], self.p.zs[q], self.p.c, :, at]
        dst = self.RH.at[q, :, at]
        return self.copy(src, dst, self.h_s.at[way, q], self.h_r.at[way, q], self.p.side(way))

    def middle(self):
        return pl.ds(self.half - self.mid, 2 * self.mid)

    def to_zmid(self, k):
        src = self.Y.at[self.p.cols[3], self.p.zs[k], self.p.c, :, self.middle()]
        return self.copy(src, self.RM.at[k - 1], self.m_s.at[k - 1], self.m_r.at[k - 1], self.p.zpeer(k))

    def beside(self, way, q, n):
        r = 2 - way
        src = self.Y.at[self.p.cols[r], self.p.zs[q], self.p.c, :, self.cols(n)]
        dst = self.RX.at[way, q, :, self.cols(n)]
        return self.copy(src, dst, self.w_s.at[way, q, n], self.w_r.at[way, q, n], self.p.side(way))

    def to_z(self, k):
        src = self.Y.at[self.p.cols[0], self.p.zs[k], self.p.c]
        return self.copy(src, self.RZ.at[k - 1], self.rz_s.at[k - 1], self.rz_r.at[k - 1], self.p.zpeer(k))

    def first(self, q, columns=(3, 1, 2, 0)):
        p = self.p
        for r in columns:
            self.pair(r, q).wait_recv()
            at = (p.cols[r], p.zs[q], p.c)
            self.Y[at] = (self.Y[at].astype(jnp.float32) + self.PR[r, q].astype(jnp.float32)).astype(jnp.bfloat16)
            if r == 3:
                if q:
                    self.to_zmid(q).start()
                else:
                    for k in (1, 2, 3):
                        self.to_zmid(k).wait_recv()
                    mid = (p.cols[r], p.zs[q], p.c, slice(None), self.middle())
                    total = self.Y[mid].astype(jnp.float32)
                    for k in range(3):
                        total = total + self.RM[k].astype(jnp.float32)
                    self.Y[mid] = total.astype(jnp.bfloat16)
                self.through(0, q).start()
                self.through(1, q).start()
            if r == 1:
                self.beside(1, q, 1).start()
            if r == 2:
                self.beside(0, q, 0).start()

    def second(self, q):
        p = self.p
        for way in (1, 0):
            n = 1 - way
            self.through(way, q).wait_recv()
            part = half_of(n, self.half, self.mid if q else 0)
            at = (p.cols[2 - way], p.zs[q], p.c, slice(None), part)
            self.Y[at] = (self.Y[at].astype(jnp.float32) + self.RH[q, :, part].astype(jnp.float32)).astype(jnp.bfloat16)
            self.beside(way, q, n).start()

    def third(self, q):
        p = self.p
        for way in (0, 1):
            for n in (0, 1):
                self.beside(way, q, n).wait_recv()
        if q:
            at = (p.cols[0], p.zs[q], p.c)
            total = self.Y[at].astype(jnp.float32) + self.RX[0, q].astype(jnp.float32) + self.RX[1, q].astype(jnp.float32)
            self.Y[at] = total.astype(jnp.bfloat16)
            self.to_z(q).start()

    def total(self):
        p = self.p
        for k in (1, 2, 3):
            self.to_z(k).wait_recv()
        at = (p.cols[0], p.zs[0], p.c)
        total = self.Y[at].astype(jnp.float32) + self.RX[0, 0].astype(jnp.float32) + self.RX[1, 0].astype(jnp.float32)
        for k in range(3):
            total = total + self.RZ[k].astype(jnp.float32)
        return total

    def finish(self):
        for k in (1, 2, 3):
            self.to_z(k).wait_send()
            self.to_zmid(k).wait_send()
        for q in range(4):
            for way in (0, 1):
                self.through(way, q).wait_send()
                for n in (0, 1):
                    self.beside(way, q, n).wait_send()
            for r in range(4):
                self.pair(r, q).wait_send()


def dot(a, b):
    return jnp.dot(a, b, preferred_element_type=jnp.float32)


def dot_t(a, b):
    return lax.dot_general(a, b, (((1,), (1,)), ((), ())), preferred_element_type=jnp.float32)


def count(shape, dim):
    return lax.broadcasted_iota(jnp.int32, shape, dim).astype(jnp.float32)


def whole(values, n):
    return jnp.floor((values + 0.5) * (1.0 / n))


def ones(mask):
    return jnp.where(mask, 1.0, 0.0).astype(jnp.bfloat16)


class Slots:
    def __init__(self, tokens, experts, cap, pieces):
        self.tokens, self.experts, self.cap, self.pieces = tokens, experts, cap, pieces
        self.each = pieces * cap
        self.slots = experts * self.each

    def of_slots(self, v):
        e = whole(v, self.each)
        rest = v - e * self.each
        j = whole(rest, self.cap)
        return e, j, rest - j * self.cap

    def of_tokens(self, v):
        j = whole(v, self.tokens)
        return j, v - j * self.tokens

    def into(self, hit_t):
        n, q = self.slots, self.pieces * self.tokens
        before = dot(hit_t, ones(count((self.tokens, self.tokens), 0) < count((self.tokens, self.tokens), 1)))
        pick = ones(self.of_slots(count((n, self.experts), 0))[0] == count((n, self.experts), 1))
        wide = ones(count((self.tokens, q), 0) == self.of_tokens(count((self.tokens, q), 1))[1])
        hits = dot(dot(pick, hit_t).astype(jnp.bfloat16), wide)
        turn = dot(dot(pick, before.astype(jnp.bfloat16)).astype(jnp.bfloat16), wide)
        e, j, slot = self.of_slots(count((n, q), 0))
        jt = self.of_tokens(count((n, q), 1))[0]
        return ones((hits > 0.5) & (turn == slot) & (j == jt))

    def out_of(self, hit, hit_k):
        n, q = self.slots, self.pieces * self.tokens
        before = dot(ones(count((self.tokens, self.tokens), 1) < count((self.tokens, self.tokens), 0)), hit)
        pick = ones(self.of_slots(count((self.experts, n), 1))[0] == count((self.experts, n), 0))
        wide = ones(count((q, self.tokens), 1) == self.of_tokens(count((q, self.tokens), 0))[1])
        e, j, slot = self.of_slots(count((q, n), 1))
        jt = self.of_tokens(count((q, n), 0))[0]
        turn = dot(wide, dot(before.astype(jnp.bfloat16), pick).astype(jnp.bfloat16))
        place = (turn == slot) & (j == jt)
        return [ones((dot(wide, dot(one, pick).astype(jnp.bfloat16)) > 0.5) & place) for one in hit_k]

    def order(self, back):
        n = self.slots
        a, b = (count((n, n), 0), count((n, n), 1)) if not back else (count((n, n), 1), count((n, n), 0))
        j = whole(a, self.experts * self.cap)
        rest = a - j * (self.experts * self.cap)
        s = whole(rest, self.cap)
        return ones(b == s * self.each + j * self.cap + (rest - s * self.cap))


def kernel(
    sections, cap, pieces,
    stream_ref, ffn_gain_ref, router_ref, ids_t_ref, wg_ref, wu_ref, wd_ref, attn_gain_ref, wkv_ref,
    out_ref, kv_ref,
    X, Y, WG, WU, WD, H, PR, RX, RH, RZ, RM, S, A, R, X2, WK, K, KR,
    local, d_s, d_r, b_s, b_r, k_s, k_r, wz_s, wz_r, wy_s, wy_r, n_s, n_r, n2_s, n2_r, np_s, np_r, *sems,
):
    p = Place()
    bf16, f32 = jnp.bfloat16, jnp.float32
    gather = Gather(p, X, sems[:11])
    reduce = Reduce(p, Y, PR, RX, RH, RZ, RM, sems[11:])
    tokens, model = stream_ref.shape
    rows = X.shape[-2]
    part = model // pieces
    cut = [slice(j * part, (j + 1) * part) for j in range(pieces)]
    slots = Slots(tokens, sections, cap, pieces)
    loads = [
        pltpu.make_async_copy(ref.at[0], buf, local.at[i])
        for i, (ref, buf) in enumerate(((wg_ref, WG), (wu_ref, WU), (wd_ref, WD)))
    ]
    for load in loads:
        load.start()
    own_wkv = pltpu.make_async_copy(wkv_ref, WK.at[p.z], local.at[3])
    own_wkv.start()

    def section(d):
        z = p.z if d % 2 == 0 else NZ - 1 - p.z
        return ((p.s + d) % sections, p.x * (NZ * 2) + z * 2 + p.c)

    def next_at(k, d):
        return ((p.s + d) % sections, p.x * (NZ * 2) + p.zs[k] * 2 + p.c)

    far = (7, 1, 5, 3, 2, 6, 4)
    barrier = pltpu.get_barrier_semaphore()
    peers = p.peers() + [section(d) for d in far]
    peers = peers + [next_at(k, d) for k in (0, 1, 2) for d in (1, sections - 1)]
    for peer in peers:
        pl.semaphore_signal(barrier, inc=1, device_id=peer, device_id_type=MESH)

    def scaled(values, gain):
        return values * lax.rsqrt(jnp.mean(values * values, axis=-1, keepdims=True) + epsilon) * gain

    normed = scaled(stream_ref[...].astype(f32), ffn_gain_ref[...]).astype(bf16)
    e_of = lax.broadcasted_iota(jnp.int32, (sections, tokens), 0)
    hit_t = ones((e_of == ids_t_ref[0:1, :]) | (e_of == ids_t_ref[1:2, :]))
    stacked = jnp.concatenate([normed[:, c] for c in cut], axis=0)
    S[...] = dot(slots.into(hit_t), stacked).astype(bf16).reshape(S.shape)

    def give(src, dst, d, send, recv):
        return pltpu.make_async_remote_copy(
            src_ref=src.at[(p.s + d) % sections], dst_ref=dst.at[p.s], send_sem=send.at[d], recv_sem=recv.at[d],
            device_id=section(d), device_id_type=MESH,
        )

    pl.semaphore_wait(barrier, len(peers))
    for d in far:
        give(S, A, d, d_s, d_r).start()
    A[p.s] = S[p.s]
    logits = dot_t(normed, router_ref[...])
    same = ones(count((tokens, tokens), 0) == count((tokens, tokens), 1))
    named = [dot_t(same, ones(e_of == ids_t_ref[k:k + 1, :])) > 0.5 for k in (0, 1)]
    chosen = [jnp.sum(jnp.where(one, logits, 0.0), axis=-1, keepdims=True) for one in named]
    share = 1.0 / (1.0 + jnp.exp(chosen[1] - chosen[0]))
    forth = slots.order(False)
    for d in far:
        give(S, A, d, d_s, d_r).wait_recv()
    block = dot(forth, A[...].reshape(slots.slots, part)).astype(bf16)
    own = (p.x, p.z, p.c)
    for j in range(pieces):
        X[p.x, p.z, p.c, :, cut[j]] = block[j * rows:(j + 1) * rows]

    gather.start()
    gather.spread_z(1)
    outer = jnp.logical_not(p.inner)
    pl.when(p.inner)(lambda: gather.spread_z(2))
    tile = min(512, model)

    y = p.s // 2
    quarter = model // 4

    def wkv_copy(z, y, send, recv, to):
        ref = WK.at[z, :, pl.ds(pl.multiple_of(y * quarter, quarter), quarter)]
        return pltpu.make_async_remote_copy(
            src_ref=ref, dst_ref=ref, send_sem=send, recv_sem=recv, device_id=to, device_id_type=MESH
        )

    def wkv_z(k, of):
        return wkv_copy(p.zs[of], y, wz_s.at[k - 1], wz_r.at[k - 1], p.zpeer(k))

    def wkv_y(k, d, of):
        return wkv_copy(p.zs[k], (y + of) % 4, wy_s.at[k - 1, d - 1], wy_r.at[k - 1, d - 1], section(2 * d))

    order = ((0, 0), (1, 0), (2, 0), (0, 1), (3, 0), (1, 1), (2, 1), (3, 1))

    def before(i):
        if i == 0:
            gather.spread_x(0)
            for load in loads:
                load.wait()
        if i == 1:
            pl.when(outer)(lambda: gather.spread_z(2))
            gather.spread_x(1)
            pl.when(p.inner)(lambda: gather.spread_z(3))
        if i == 2:
            gather.spread_x2(0)
        if i == 3:
            pl.when(outer)(lambda: gather.spread_z(3))
            gather.spread_x(2)
        if i == 4:
            gather.spread_x2(1)
        if i == 5:
            gather.spread_x(3)
            own_wkv.wait()
            for k in (1, 2, 3):
                wkv_z(k, 0).start()
        if i == 6:
            for q in (1, 0):
                reduce.first(q, (1, 2))
        if i == 7:
            gather.spread_x2(2)
            gather.spread_x2(3)
        r, b = order[i]
        gather.need(r, (2 * b, 2 * b + 1))

    def behind(i):
        r, b = order[i]
        for q in (2 * b, 2 * b + 1):
            reduce.pair(r, q).start()

    def step(i, carry):
        for n in range(8):
            pl.when(i == n)(functools.partial(before, n))
        r = (i == 1) * 1 + (i == 2) * 2 + (i == 4) * 3 + (i == 5) * 1 + (i == 6) * 2 + (i == 7) * 3
        b = (i == 3) * 1 + (i >= 5) * 1
        shift = (r == 1) * 3 + (r == 2) * 1 + (r == 3) * 2
        col = (p.x + shift) % NX
        pair = (p.z // 2 + b) % 2
        zs = pl.ds(2 * pair, 2)
        value = X[col, zs].reshape(4 * rows, model)
        gate = dot_t(value, WG[...])
        up = dot_t(value, WU[...])
        H[...] = (gate / (1.0 + jnp.exp(-gate)) * up).astype(bf16)

        def down(n, carry):
            at = pl.ds(pl.multiple_of(n * tile, tile), tile)
            Y[col, zs, :, :, at] = dot(H[...], WD[:, at]).astype(bf16).reshape(2, 2, rows, tile)
            return carry

        lax.fori_loop(0, model // tile, down, 0)
        for n in range(8):
            pl.when(i == n)(functools.partial(behind, n))
        return carry

    lax.fori_loop(0, 8, step, 0)
    reduce.first(2)
    reduce.second(2)
    reduce.first(3)
    reduce.third(2)
    reduce.second(3)
    reduce.first(1, (3, 0))
    reduce.third(3)
    reduce.first(0, (3, 0))
    reduce.second(1)
    for k in (1, 2, 3):
        wkv_z(k, k).wait_recv()
        for d in (1, 2, 3):
            wkv_y(k, d, 0).start()
    reduce.second(0)
    reduce.third(1)
    reduce.third(0)
    hit_k = [ones(one) for one in named]
    fetch = slots.out_of(ones(named[0] | named[1]), hit_k)
    sums = reduce.total().astype(bf16)
    for d in far:
        give(S, A, d, d_s, d_r).wait_send()
    packed = dot(slots.order(True), jnp.concatenate([sums[:, c] for c in cut], axis=0)).astype(bf16)
    S[...] = packed.reshape(S.shape)
    for d in far:
        give(S, R, d, b_s, b_r).start()
    R[p.s] = S[p.s]
    for d in far:
        give(S, R, d, b_s, b_r).wait_recv()
    back = R[...].reshape(slots.slots, part)
    share = jnp.concatenate([share] * pieces, axis=0)
    base = jnp.concatenate([stream_ref[:, c].astype(f32) for c in cut], axis=0)
    updated = (base + share * dot(fetch[0], back) + (1.0 - share) * dot(fetch[1], back)).astype(bf16)
    floats = updated.astype(f32)
    squares = jnp.sum(floats * floats, axis=-1, keepdims=True)
    total = squares[0:tokens]
    for j in range(1, pieces):
        total = total + squares[j * tokens:(j + 1) * tokens]
    scale = lax.rsqrt(total * (1.0 / model) + epsilon)
    for j in range(pieces):
        at = slice(j * tokens, (j + 1) * tokens)
        X2[p.x, p.c, :, cut[j]] = (floats[at] * scale * attn_gain_ref[:, cut[j]]).astype(bf16)

    half = model // 2

    def row(c, r, at, send, recv, to):
        ref = X2.at[p.cols[r], c, :, at]
        return pltpu.make_async_remote_copy(
            src_ref=ref, dst_ref=ref, send_sem=send, recv_sem=recv, device_id=to, device_id_type=MESH
        )

    every = pl.ds(0, model)

    def row_x(way, r):
        return row(p.c, r, every, n_s.at[way], n_r.at[way], p.side(way))

    def row_x2(way, r):
        return row(p.c, r, pl.ds(way * half, half), n2_s.at[way], n2_r.at[way], p.side(way))

    def row_pair(r, c):
        return row(c, r, every, np_s.at[r], np_r.at[r], p.partner())

    for way in (0, 1):
        row_x(way, 0).start()
    row_pair(0, p.c).start()
    for j in range(pieces):
        out_ref[:, cut[j]] = updated[j * tokens:(j + 1) * tokens]
    for way in (0, 1):
        row_x(way, 1 + way).wait_recv()
        row_x2(way, 1 + way).start()
    for way in (0, 1):
        row_pair(1 + way, p.c).start()
    for k in (1, 2, 3):
        for d in (1, 2, 3):
            wkv_y(k, d, 4 - d).wait_recv()
    for way in (0, 1):
        row_x2(way, 3).wait_recv()
    row_pair(3, p.c).start()
    for r in range(4):
        row_pair(r, 1 - p.c).wait_recv()
    width = WK.shape[1]
    each = NX * 2 * tokens
    K[...] = dot_t(WK[...].reshape(NZ * width, model), X2[...].reshape(each, model)).astype(bf16).reshape(K.shape)

    def piece(k):
        return pltpu.make_async_remote_copy(
            src_ref=K.at[p.zs[k]], dst_ref=KR.at[p.z], send_sem=k_s.at[k], recv_sem=k_r.at[k],
            device_id=next_at(k, 1), device_id_type=MESH,
        )

    for k in (3, 1, 2, 0):
        piece(k).start()
    a, b = count((NZ * each, NZ * each), 0), count((NZ * each, NZ * each), 1)
    z_of = whole(a, each)
    x_of = whole(a - z_of * each, 2 * tokens)
    t_of = a - z_of * each - x_of * (2 * tokens)
    into = ones(b == x_of * each + z_of * (2 * tokens) + t_of)
    for k in range(4):
        piece(k).wait_recv()
    kv_ref[...] = dot(jnp.concatenate([KR[z] for z in range(NZ)], axis=1), into).astype(bf16)
    gather.finish()
    reduce.finish()
    for k in (1, 2, 3):
        wkv_z(k, 0).wait_send()
        for d in (1, 2, 3):
            wkv_y(k, d, 0).wait_send()
    for d in far:
        give(S, R, d, b_s, b_r).wait_send()
    for way in (0, 1):
        row_x(way, 0).wait_send()
        row_x2(way, 1 + way).wait_send()
    for r in range(4):
        row_pair(r, p.c).wait_send()
        piece(r).wait_send()


def body(stream, ffn_gain, router_weight, expert_ids, w_gate, w_up, w_down, attn_gain, w_kv):
    tokens, model = stream.shape
    sections = lax.axis_size("section")
    cap = min(tokens, 3 * tokens // router_weight.shape[1])
    pieces = 8
    rows = sections * cap
    hidden = w_gate.shape[-1]
    width = w_kv.shape[1]
    part = model // pieces
    bf16 = jnp.bfloat16
    dma = pltpu.SemaphoreType.DMA
    any_space = pl.BlockSpec(memory_space=pl.ANY)
    vmem = pl.BlockSpec(memory_space=pltpu.VMEM)
    exchange = pltpu.VMEM((sections, pieces * cap, part), bf16)
    stream_out, kv_t = pl.pallas_call(
        functools.partial(kernel, sections, cap, pieces),
        out_shape=(
            jax.ShapeDtypeStruct((tokens, model), bf16),
            jax.ShapeDtypeStruct((width, NX * NZ * 2 * tokens), bf16),
        ),
        in_specs=[vmem] * 4 + [any_space] * 3 + [vmem, any_space],
        out_specs=(vmem, vmem),
        scratch_shapes=[
            pltpu.VMEM((NX, NZ, 2, rows, model), bf16),
            pltpu.VMEM((NX, NZ, 2, rows, model), bf16),
            pltpu.VMEM((hidden, model), bf16),
            pltpu.VMEM((hidden, model), bf16),
            pltpu.VMEM((hidden, model), bf16),
            pltpu.VMEM((4 * rows, hidden), bf16),
            pltpu.VMEM((4, 4, rows, model), bf16),
            pltpu.VMEM((2, 4, rows, model), bf16),
            pltpu.VMEM((4, rows, model), bf16),
            pltpu.VMEM((3, rows, model), bf16),
            pltpu.VMEM((3, rows, 2 * mid_of(model)), bf16),
            exchange,
            exchange,
            exchange,
            pltpu.VMEM((NX, 2, tokens, model), bf16),
            pltpu.VMEM((NZ, width, model), bf16),
            pltpu.VMEM((NZ, width, NX * 2 * tokens), bf16),
            pltpu.VMEM((NZ, width, NX * 2 * tokens), bf16),
            dma((4,)),
            dma((8,)), dma((8,)), dma((8,)), dma((8,)),
            dma((4,)), dma((4,)),
            dma((3,)), dma((3,)), dma((3, 3)), dma((3, 3)),
            dma((2,)), dma((2,)), dma((2,)), dma((2,)), dma((4,)), dma((4,)),
            *Gather.sems(),
            *Reduce.sems(),
        ],
        compiler_params=pltpu.CompilerParams(
            collective_id=0, has_side_effects=True, vmem_limit_bytes=VMEM_LIMIT
        ),
        name="layer",
    )(
        stream, ffn_gain[None, :], router_weight.T, expert_ids.T,
        jnp.swapaxes(w_gate, 1, 2), jnp.swapaxes(w_up, 1, 2), w_down, attn_gain[None, :], w_kv.T,
    )
    return (stream_out, kv_t.T)


def solution(mesh):
    in_specs = (
        P(("section", "mp"), None),
        P(),
        P(),
        P(("section", "mp"), None),
        P("section", None, "mp"),
        P("section", None, "mp"),
        P("section", "mp", None),
        P(),
        P(None, "mp"),
    )
    out_specs = (P(("section", "mp"), None), P("section", "mp"))
    return jax.shard_map(body, mesh=mesh, in_specs=in_specs, out_specs=out_specs, check_vma=False)
```

```python
import functools

import jax
import jax.numpy as jnp
from jax import lax
from jax.experimental import pallas as pl
from jax.experimental.pallas import tpu as pltpu
from jax.sharding import PartitionSpec as P

epsilon = 1e-05
MESH = pl.DeviceIdType.MESH
NX = 4
NZ = 4
VMEM_LIMIT = 66_000_000


class Place:
    def __init__(self):
        self.s = lax.axis_index("section")
        m = lax.axis_index("mp")
        self.x = m // (NZ * 2)
        self.z = (m // 2) % NZ
        self.c = m % 2
        z = self.z
        self.cols = [self.x, (self.x + 3) % NX, (self.x + 1) % NX, (self.x + 2) % NX]
        self.zs = [z, z + 1 - 2 * (z % 2), (z + 2) % NZ, NZ - 1 - z]
        self.inner = (z == 1) | (z == 2)
        self.zq = [z, z + 1 - 2 * (z % 2), 2 - z // 2, 3 - 3 * (z // 2)]

    def at(self, x, z, c):
        return (self.s, x * (NZ * 2) + z * 2 + c)

    def partner(self):
        return self.at(self.x, self.z, 1 - self.c)

    def side(self, way):
        return self.at(self.cols[2 - way], self.z, self.c)

    def zpeer(self, k):
        return self.at(self.x, self.zs[k], self.c)

    def peers(self):
        return [self.partner(), self.side(0), self.side(1)] + [self.zpeer(k) for k in (1, 2, 3)]


def mid_of(model):
    return model * 5 // 32


def far_of(model):
    return model // 32 * 6


def half_of(way, half, mid):
    return pl.ds(way * (half + mid), half - mid)


class Gather:
    def __init__(self, place, X, sems):
        self.p, self.X = place, X
        self.zo_s, self.zf_s, self.zs_r, self.xs_s, self.xs_r, self.x2_s, self.x2_r, self.p_s, self.p_r, self.m_s, self.m_r = sems
        self.half = X.shape[-1] // 2
        self.mid = far_of(X.shape[-1])

    @staticmethod
    def sems():
        dma = pltpu.SemaphoreType.DMA
        return [
            dma((2,)), dma((3,)), dma((3,)), dma((2, 4)), dma((2, 4)), dma((2, 4)), dma((2, 4)), dma((4, 4)), dma((4, 4)),
            dma((3,)), dma((3,)),
        ]

    def block(self, r, q, c):
        return self.X.at[self.p.cols[r], self.p.zq[q], c]

    def copy(self, ref, send, recv, to):
        return pltpu.make_async_remote_copy(
            src_ref=ref, dst_ref=ref, send_sem=send, recv_sem=recv, device_id=to, device_id_type=MESH
        )

    def own_z(self, n):
        return self.copy(self.block(0, 0, self.p.c), self.zo_s.at[n], self.zs_r.at[n], self.p.at(self.p.x, self.p.zq[1 + n], self.p.c))

    def on_z(self, q):
        to, kind = (2, 3) if q == 1 else (1, q)
        return self.copy(self.block(0, q, self.p.c), self.zf_s.at[q - 1], self.zs_r.at[kind - 1], self.p.at(self.p.x, self.p.zq[to], self.p.c))

    def from_z(self, q):
        return self.copy(self.block(0, q, self.p.c), self.zf_s.at[q - 1], self.zs_r.at[q - 1], self.p.partner())

    def to_x(self, way, q):
        return self.copy(self.block(0, q, self.p.c), self.xs_s.at[way, q], self.xs_r.at[way, q], self.p.side(way))

    def from_x(self, way, q):
        return self.copy(self.block(1 + way, q, self.p.c), self.xs_s.at[way, q], self.xs_r.at[way, q], self.p.side(way))

    def part(self, r, q, way):
        return self.X.at[self.p.cols[r], self.p.zq[q], self.p.c, :, half_of(way, self.half, self.mid if q else 0)]

    def to_zmid(self, k):
        ref = self.X.at[self.p.cols[3], self.p.zs[0], self.p.c, :, pl.ds(self.half - self.mid, 2 * self.mid)]
        return self.copy(ref, self.m_s.at[k - 1], self.m_r.at[k - 1], self.p.zpeer(k))

    def from_zmid(self, k):
        ref = self.X.at[self.p.cols[3], self.p.zs[k], self.p.c, :, pl.ds(self.half - self.mid, 2 * self.mid)]
        return self.copy(ref, self.m_s.at[k - 1], self.m_r.at[k - 1], self.p.zpeer(k))

    def on_x(self, way, q):
        return self.copy(self.part(1 + way, q, way), self.x2_s.at[way, q], self.x2_r.at[way, q], self.p.side(way))

    def from_x2(self, way, q):
        return self.copy(self.part(3, q, way), self.x2_s.at[way, q], self.x2_r.at[way, q], self.p.side(way))

    def pair(self, r, q):
        return self.copy(self.block(r, q, self.p.c), self.p_s.at[r, q], self.p_r.at[r, q], self.p.partner())

    def from_pair(self, r, q):
        return self.copy(self.block(r, q, 1 - self.p.c), self.p_s.at[r, q], self.p_r.at[r, q], self.p.partner())

    def start(self):
        self.to_x(0, 0).start()
        self.to_x(1, 0).start()
        self.own_z(0).start()
        pl.when(self.p.inner)(lambda: self.own_z(1).start())
        self.pair(0, 0).start()

    def spread_z(self, k):
        self.from_z(k).wait_recv()
        pl.when(self.p.inner)(lambda: self.on_z(k).start())
        self.to_x(0, k).start()
        self.to_x(1, k).start()
        self.pair(0, k).start()

    def spread_x(self, q):
        for way in (0, 1):
            self.from_x(way, q).wait_recv()
            self.on_x(way, q).start()
        for way in (0, 1):
            self.pair(1 + way, q).start()

    def spread_x2(self, q):
        for way in (0, 1):
            self.from_x2(way, q).wait_recv()
        if q == 0:
            for k in (1, 2, 3):
                self.to_zmid(k).start()
        if q == 1:
            self.from_zmid(1).wait_recv()
        if q < 2:
            self.pair(3, q).start()
        if q == 3:
            for k in (2, 3):
                self.from_zmid(k).wait_recv()
            for k in (2, 3):
                self.pair(3, k).start()

    def need(self, r, qs):
        for q in qs:
            self.from_pair(r, q).wait_recv()

    def finish(self):
        self.own_z(0).wait_send()

        def inner():
            self.own_z(1).wait_send()
            for q in (1, 2, 3):
                self.on_z(q).wait_send()

        pl.when(self.p.inner)(inner)
        for k in (1, 2, 3):
            self.to_zmid(k).wait_send()
        for q in range(4):
            for way in (0, 1):
                self.to_x(way, q).wait_send()
                self.on_x(way, q).wait_send()
            for r in range(4):
                self.pair(r, q).wait_send()


def enter(peers):
    barrier = pltpu.get_barrier_semaphore()
    for peer in peers:
        pl.semaphore_signal(barrier, inc=1, device_id=peer, device_id_type=MESH)
    pl.semaphore_wait(barrier, len(peers))


class Reduce:
    def __init__(self, place, Y, PR, RX, RH, RZ, RM, sems):
        self.p, self.Y, self.PR, self.RX, self.RH, self.RZ, self.RM = place, Y, PR, RX, RH, RZ, RM
        self.py_s, self.py_r, self.h_s, self.h_r, self.w_s, self.w_r, self.rz_s, self.rz_r, self.m_s, self.m_r = sems
        self.half = Y.shape[-1] // 2
        self.mid = mid_of(Y.shape[-1])

    @staticmethod
    def sems():
        dma = pltpu.SemaphoreType.DMA
        return [
            dma((4, 4)), dma((4, 4)), dma((2, 4)), dma((2, 4)), dma((2, 4, 2)), dma((2, 4, 2)), dma((3,)), dma((3,)),
            dma((3,)), dma((3,)),
        ]

    def copy(self, src, dst, send, recv, to):
        return pltpu.make_async_remote_copy(
            src_ref=src, dst_ref=dst, send_sem=send, recv_sem=recv, device_id=to, device_id_type=MESH
        )

    def pair(self, r, q):
        src = self.Y.at[self.p.cols[r], self.p.zs[q], 1 - self.p.c]
        return self.copy(src, self.PR.at[r, q], self.py_s.at[r, q], self.py_r.at[r, q], self.p.partner())

    def cols(self, n):
        return pl.ds(n * self.half, self.half)

    def through(self, way, q):
        at = half_of(1 - way, self.half, self.mid if q else 0)
        src = self.Y.at[self.p.cols[3], self.p.zs[q], self.p.c, :, at]
        dst = self.RH.at[q, :, at]
        return self.copy(src, dst, self.h_s.at[way, q], self.h_r.at[way, q], self.p.side(way))

    def middle(self):
        return pl.ds(self.half - self.mid, 2 * self.mid)

    def to_zmid(self, k):
        src = self.Y.at[self.p.cols[3], self.p.zs[k], self.p.c, :, self.middle()]
        return self.copy(src, self.RM.at[k - 1], self.m_s.at[k - 1], self.m_r.at[k - 1], self.p.zpeer(k))

    def beside(self, way, q, n):
        r = 2 - way
        src = self.Y.at[self.p.cols[r], self.p.zs[q], self.p.c, :, self.cols(n)]
        dst = self.RX.at[way, q, :, self.cols(n)]
        return self.copy(src, dst, self.w_s.at[way, q, n], self.w_r.at[way, q, n], self.p.side(way))

    def to_z(self, k):
        src = self.Y.at[self.p.cols[0], self.p.zs[k], self.p.c]
        return self.copy(src, self.RZ.at[k - 1], self.rz_s.at[k - 1], self.rz_r.at[k - 1], self.p.zpeer(k))

    def first(self, q, columns=(3, 1, 2, 0)):
        p = self.p
        for r in columns:
            self.pair(r, q).wait_recv()
            at = (p.cols[r], p.zs[q], p.c)
            self.Y[at] = (self.Y[at].astype(jnp.float32) + self.PR[r, q].astype(jnp.float32)).astype(jnp.bfloat16)
            if r == 3:
                if q:
                    self.to_zmid(q).start()
                else:
                    for k in (1, 2, 3):
                        self.to_zmid(k).wait_recv()
                    mid = (p.cols[r], p.zs[q], p.c, slice(None), self.middle())
                    total = self.Y[mid].astype(jnp.float32)
                    for k in range(3):
                        total = total + self.RM[k].astype(jnp.float32)
                    self.Y[mid] = total.astype(jnp.bfloat16)
                self.through(0, q).start()
                self.through(1, q).start()
            if r == 1:
                self.beside(1, q, 1).start()
            if r == 2:
                self.beside(0, q, 0).start()

    def second(self, q):
        p = self.p
        for way in (1, 0):
            n = 1 - way
            self.through(way, q).wait_recv()
            part = half_of(n, self.half, self.mid if q else 0)
            at = (p.cols[2 - way], p.zs[q], p.c, slice(None), part)
            self.Y[at] = (self.Y[at].astype(jnp.float32) + self.RH[q, :, part].astype(jnp.float32)).astype(jnp.bfloat16)
            self.beside(way, q, n).start()

    def third(self, q):
        p = self.p
        for way in (0, 1):
            for n in (0, 1):
                self.beside(way, q, n).wait_recv()
        if q:
            at = (p.cols[0], p.zs[q], p.c)
            total = self.Y[at].astype(jnp.float32) + self.RX[0, q].astype(jnp.float32) + self.RX[1, q].astype(jnp.float32)
            self.Y[at] = total.astype(jnp.bfloat16)
            self.to_z(q).start()

    def total(self):
        p = self.p
        for k in (1, 2, 3):
            self.to_z(k).wait_recv()
        at = (p.cols[0], p.zs[0], p.c)
        total = self.Y[at].astype(jnp.float32) + self.RX[0, 0].astype(jnp.float32) + self.RX[1, 0].astype(jnp.float32)
        for k in range(3):
            total = total + self.RZ[k].astype(jnp.float32)
        return total

    def finish(self):
        for k in (1, 2, 3):
            self.to_z(k).wait_send()
            self.to_zmid(k).wait_send()
        for q in range(4):
            for way in (0, 1):
                self.through(way, q).wait_send()
                for n in (0, 1):
                    self.beside(way, q, n).wait_send()
            for r in range(4):
                self.pair(r, q).wait_send()


def dot(a, b):
    return jnp.dot(a, b, preferred_element_type=jnp.float32)


def dot_t(a, b):
    return lax.dot_general(a, b, (((1,), (1,)), ((), ())), preferred_element_type=jnp.float32)


def count(shape, dim):
    return lax.broadcasted_iota(jnp.int32, shape, dim).astype(jnp.float32)


def whole(values, n):
    return jnp.floor((values + 0.5) * (1.0 / n))


def ones(mask):
    return jnp.where(mask, 1.0, 0.0).astype(jnp.bfloat16)


class Slots:
    def __init__(self, tokens, experts, cap, pieces):
        self.tokens, self.experts, self.cap, self.pieces = tokens, experts, cap, pieces
        self.each = pieces * cap
        self.slots = experts * self.each

    def of_slots(self, v):
        e = whole(v, self.each)
        rest = v - e * self.each
        j = whole(rest, self.cap)
        return e, j, rest - j * self.cap

    def of_tokens(self, v):
        j = whole(v, self.tokens)
        return j, v - j * self.tokens

    def into(self, hit_t):
        n, q = self.slots, self.pieces * self.tokens
        before = dot(hit_t, ones(count((self.tokens, self.tokens), 0) < count((self.tokens, self.tokens), 1)))
        pick = ones(self.of_slots(count((n, self.experts), 0))[0] == count((n, self.experts), 1))
        wide = ones(count((self.tokens, q), 0) == self.of_tokens(count((self.tokens, q), 1))[1])
        hits = dot(dot(pick, hit_t).astype(jnp.bfloat16), wide)
        turn = dot(dot(pick, before.astype(jnp.bfloat16)).astype(jnp.bfloat16), wide)
        e, j, slot = self.of_slots(count((n, q), 0))
        jt = self.of_tokens(count((n, q), 1))[0]
        return ones((hits > 0.5) & (turn == slot) & (j == jt))

    def out_of(self, hit, hit_k):
        n, q = self.slots, self.pieces * self.tokens
        before = dot(ones(count((self.tokens, self.tokens), 1) < count((self.tokens, self.tokens), 0)), hit)
        pick = ones(self.of_slots(count((self.experts, n), 1))[0] == count((self.experts, n), 0))
        wide = ones(count((q, self.tokens), 1) == self.of_tokens(count((q, self.tokens), 0))[1])
        e, j, slot = self.of_slots(count((q, n), 1))
        jt = self.of_tokens(count((q, n), 0))[0]
        turn = dot(wide, dot(before.astype(jnp.bfloat16), pick).astype(jnp.bfloat16))
        place = (turn == slot) & (j == jt)
        return [ones((dot(wide, dot(one, pick).astype(jnp.bfloat16)) > 0.5) & place) for one in hit_k]

    def order(self, back):
        n = self.slots
        a, b = (count((n, n), 0), count((n, n), 1)) if not back else (count((n, n), 1), count((n, n), 0))
        j = whole(a, self.experts * self.cap)
        rest = a - j * (self.experts * self.cap)
        s = whole(rest, self.cap)
        return ones(b == s * self.each + j * self.cap + (rest - s * self.cap))


def kernel(
    sections, cap, pieces,
    stream_ref, ffn_gain_ref, router_ref, ids_t_ref, wg_ref, wu_ref, wd_ref, attn_gain_ref, wkv_ref,
    out_ref, kv_ref,
    X, Y, WG, WU, WD, H, PR, RX, RH, RZ, RM, S, A, R, X2, WK, K, KR,
    local, d_s, d_r, b_s, b_r, k_s, k_r, wz_s, wz_r, wy_s, wy_r, n_s, n_r, n2_s, n2_r, np_s, np_r, *sems,
):
    p = Place()
    bf16, f32 = jnp.bfloat16, jnp.float32
    gather = Gather(p, X, sems[:11])
    reduce = Reduce(p, Y, PR, RX, RH, RZ, RM, sems[11:])
    tokens, model = stream_ref.shape
    rows = X.shape[-2]
    part = model // pieces
    cut = [slice(j * part, (j + 1) * part) for j in range(pieces)]
    slots = Slots(tokens, sections, cap, pieces)
    loads = [
        pltpu.make_async_copy(ref.at[0], buf, local.at[i])
        for i, (ref, buf) in enumerate(((wg_ref, WG), (wu_ref, WU), (wd_ref, WD)))
    ]
    for load in loads:
        load.start()
    own_wkv = pltpu.make_async_copy(wkv_ref, WK.at[p.z], local.at[3])
    own_wkv.start()

    def section(d):
        z = p.z if d % 2 == 0 else NZ - 1 - p.z
        return ((p.s + d) % sections, p.x * (NZ * 2) + z * 2 + p.c)

    def next_at(k, d):
        return ((p.s + d) % sections, p.x * (NZ * 2) + p.zs[k] * 2 + p.c)

    far = (7, 1, 5, 3, 2, 6, 4)
    barrier = pltpu.get_barrier_semaphore()
    peers = p.peers() + [section(d) for d in far]
    peers = peers + [next_at(k, d) for k in (0, 1, 2) for d in (1, sections - 1)]
    for peer in peers:
        pl.semaphore_signal(barrier, inc=1, device_id=peer, device_id_type=MESH)

    def scaled(values, gain):
        return values * lax.rsqrt(jnp.mean(values * values, axis=-1, keepdims=True) + epsilon) * gain

    normed = scaled(stream_ref[...].astype(f32), ffn_gain_ref[...]).astype(bf16)
    e_of = lax.broadcasted_iota(jnp.int32, (sections, tokens), 0)
    hit_t = ones((e_of == ids_t_ref[0:1, :]) | (e_of == ids_t_ref[1:2, :]))
    stacked = jnp.concatenate([normed[:, c] for c in cut], axis=0)
    S[...] = dot(slots.into(hit_t), stacked).astype(bf16).reshape(S.shape)

    def give(src, dst, d, send, recv):
        return pltpu.make_async_remote_copy(
            src_ref=src.at[(p.s + d) % sections], dst_ref=dst.at[p.s], send_sem=send.at[d], recv_sem=recv.at[d],
            device_id=section(d), device_id_type=MESH,
        )

    pl.semaphore_wait(barrier, len(peers))
    for d in far:
        give(S, A, d, d_s, d_r).start()
    A[p.s] = S[p.s]
    logits = dot_t(normed, router_ref[...])
    same = ones(count((tokens, tokens), 0) == count((tokens, tokens), 1))
    named = [dot_t(same, ones(e_of == ids_t_ref[k:k + 1, :])) > 0.5 for k in (0, 1)]
    chosen = [jnp.sum(jnp.where(one, logits, 0.0), axis=-1, keepdims=True) for one in named]
    share = 1.0 / (1.0 + jnp.exp(chosen[1] - chosen[0]))
    forth = slots.order(False)
    for d in far:
        give(S, A, d, d_s, d_r).wait_recv()
    block = dot(forth, A[...].reshape(slots.slots, part)).astype(bf16)
    own = (p.x, p.z, p.c)
    for j in range(pieces):
        X[p.x, p.z, p.c, :, cut[j]] = block[j * rows:(j + 1) * rows]

    gather.start()
    gather.spread_z(1)
    outer = jnp.logical_not(p.inner)
    pl.when(p.inner)(lambda: gather.spread_z(2))
    tile = min(512, model)

    y = p.s // 2
    quarter = model // 4

    def wkv_copy(z, y, send, recv, to):
        ref = WK.at[z, :, pl.ds(pl.multiple_of(y * quarter, quarter), quarter)]
        return pltpu.make_async_remote_copy(
            src_ref=ref, dst_ref=ref, send_sem=send, recv_sem=recv, device_id=to, device_id_type=MESH
        )

    def wkv_z(k, of):
        return wkv_copy(p.zs[of], y, wz_s.at[k - 1], wz_r.at[k - 1], p.zpeer(k))

    def wkv_y(k, d, of):
        return wkv_copy(p.zs[k], (y + of) % 4, wy_s.at[k - 1, d - 1], wy_r.at[k - 1, d - 1], section(2 * d))

    order = (((0, 0), (1, 0)), ((2, 0), (0, 1)), ((3, 0), (1, 1)), ((2, 1), (3, 1)))

    def before(i):
        if i == 0:
            gather.spread_x(0)
            for load in loads:
                load.wait()
            pl.when(outer)(lambda: gather.spread_z(2))
            gather.spread_x(1)
            pl.when(p.inner)(lambda: gather.spread_z(3))
        if i == 1:
            gather.spread_x2(0)
            pl.when(outer)(lambda: gather.spread_z(3))
            gather.spread_x(2)
        if i == 2:
            gather.spread_x2(1)
            gather.spread_x(3)
            own_wkv.wait()
            for k in (1, 2, 3):
                wkv_z(k, 0).start()
        if i == 3:
            gather.spread_x2(2)
            gather.spread_x2(3)
            for q in (1, 0):
                reduce.first(q, (1, 2))
        for r, b in order[i]:
            gather.need(r, (2 * b, 2 * b + 1))

    def behind(i):
        for n in (0, 1):
            for r, b in reversed(order[i]):
                reduce.pair(r, 2 * b + n).start()

    def step(i, carry):
        for n in range(4):
            pl.when(i == n)(functools.partial(before, n))
        halves = []
        for n in (0, 1):
            shift = sum((i == k) * (0, 3, 1, 2)[order[k][n][0]] for k in range(4))
            far_pair = sum((i == k) * order[k][n][1] for k in range(4))
            halves.append(((p.x + shift) % NX, pl.ds(2 * ((p.z // 2 + far_pair) % 2), 2)))
        value = jnp.concatenate([X[col, zs].reshape(4 * rows, model) for col, zs in halves], axis=0)
        gate = dot_t(value, WG[...])
        up = dot_t(value, WU[...])
        H[...] = (gate / (1.0 + jnp.exp(-gate)) * up).astype(bf16)

        def down(n, carry):
            at = pl.ds(pl.multiple_of(n * tile, tile), tile)
            part = dot(H[...], WD[:, at]).astype(bf16)
            for k, (col, zs) in enumerate(halves):
                Y[col, zs, :, :, at] = part[k * 4 * rows:(k + 1) * 4 * rows].reshape(2, 2, rows, tile)
            return carry

        lax.fori_loop(0, model // tile, down, 0)
        for n in range(4):
            pl.when(i == n)(functools.partial(behind, n))
        return carry

    lax.fori_loop(0, 4, step, 0)
    reduce.first(2)
    reduce.second(2)
    reduce.first(3)
    reduce.third(2)
    reduce.second(3)
    reduce.first(1, (3, 0))
    reduce.third(3)
    reduce.first(0, (3, 0))
    reduce.second(1)
    backward = slots.order(True)
    fetch = slots.out_of(ones(named[0] | named[1]), [ones(one) for one in named])
    for k in (1, 2, 3):
        wkv_z(k, k).wait_recv()
        for d in (1, 2, 3):
            wkv_y(k, d, 0).start()
    reduce.second(0)
    reduce.third(1)
    reduce.third(0)
    sums = reduce.total().astype(bf16)
    for d in far:
        give(S, A, d, d_s, d_r).wait_send()
    packed = dot(backward, jnp.concatenate([sums[:, c] for c in cut], axis=0)).astype(bf16)
    S[...] = packed.reshape(S.shape)
    for d in far:
        give(S, R, d, b_s, b_r).start()
    R[p.s] = S[p.s]
    for d in far:
        give(S, R, d, b_s, b_r).wait_recv()
    back = R[...].reshape(slots.slots, part)
    share = jnp.concatenate([share] * pieces, axis=0)
    base = jnp.concatenate([stream_ref[:, c].astype(f32) for c in cut], axis=0)
    updated = (base + share * dot(fetch[0], back) + (1.0 - share) * dot(fetch[1], back)).astype(bf16)
    floats = updated.astype(f32)
    squares = jnp.sum(floats * floats, axis=-1, keepdims=True)
    total = squares[0:tokens]
    for j in range(1, pieces):
        total = total + squares[j * tokens:(j + 1) * tokens]
    scale = lax.rsqrt(total * (1.0 / model) + epsilon)
    for j in range(pieces):
        at = slice(j * tokens, (j + 1) * tokens)
        X2[p.x, p.c, :, cut[j]] = (floats[at] * scale * attn_gain_ref[:, cut[j]]).astype(bf16)

    half = model // 2

    def row(c, r, at, send, recv, to):
        ref = X2.at[p.cols[r], c, :, at]
        return pltpu.make_async_remote_copy(
            src_ref=ref, dst_ref=ref, send_sem=send, recv_sem=recv, device_id=to, device_id_type=MESH
        )

    every = pl.ds(0, model)

    def row_x(way, r):
        return row(p.c, r, every, n_s.at[way], n_r.at[way], p.side(way))

    def row_x2(way, r):
        return row(p.c, r, pl.ds(way * half, half), n2_s.at[way], n2_r.at[way], p.side(way))

    def row_pair(r, c):
        return row(c, r, every, np_s.at[r], np_r.at[r], p.partner())

    for way in (0, 1):
        row_x(way, 0).start()
    row_pair(0, p.c).start()
    for j in range(pieces):
        out_ref[:, cut[j]] = updated[j * tokens:(j + 1) * tokens]
    for way in (0, 1):
        row_x(way, 1 + way).wait_recv()
        row_x2(way, 1 + way).start()
    for way in (0, 1):
        row_pair(1 + way, p.c).start()
    for k in (1, 2, 3):
        for d in (1, 2, 3):
            wkv_y(k, d, 4 - d).wait_recv()
    for way in (0, 1):
        row_x2(way, 3).wait_recv()
    row_pair(3, p.c).start()
    for r in range(4):
        row_pair(r, 1 - p.c).wait_recv()
    width = WK.shape[1]
    each = NX * 2 * tokens
    K[...] = dot_t(WK[...].reshape(NZ * width, model), X2[...].reshape(each, model)).astype(bf16).reshape(K.shape)

    def piece(k):
        return pltpu.make_async_remote_copy(
            src_ref=K.at[p.zs[k]], dst_ref=KR.at[p.z], send_sem=k_s.at[k], recv_sem=k_r.at[k],
            device_id=next_at(k, 1), device_id_type=MESH,
        )

    for k in (3, 1, 2, 0):
        piece(k).start()
    a, b = count((NZ * each, NZ * each), 0), count((NZ * each, NZ * each), 1)
    z_of = whole(a, each)
    x_of = whole(a - z_of * each, 2 * tokens)
    t_of = a - z_of * each - x_of * (2 * tokens)
    into = ones(b == x_of * each + z_of * (2 * tokens) + t_of)
    for k in range(4):
        piece(k).wait_recv()
    kv_ref[...] = dot(jnp.concatenate([KR[z] for z in range(NZ)], axis=1), into).astype(bf16)
    gather.finish()
    reduce.finish()
    for k in (1, 2, 3):
        wkv_z(k, 0).wait_send()
        for d in (1, 2, 3):
            wkv_y(k, d, 0).wait_send()
    for d in far:
        give(S, R, d, b_s, b_r).wait_send()
    for way in (0, 1):
        row_x(way, 0).wait_send()
        row_x2(way, 1 + way).wait_send()
    for r in range(4):
        row_pair(r, p.c).wait_send()
        piece(r).wait_send()


def body(stream, ffn_gain, router_weight, expert_ids, w_gate, w_up, w_down, attn_gain, w_kv):
    tokens, model = stream.shape
    sections = lax.axis_size("section")
    cap = min(tokens, 3 * tokens // router_weight.shape[1])
    pieces = 8
    rows = sections * cap
    hidden = w_gate.shape[-1]
    width = w_kv.shape[1]
    part = model // pieces
    bf16 = jnp.bfloat16
    dma = pltpu.SemaphoreType.DMA
    any_space = pl.BlockSpec(memory_space=pl.ANY)
    vmem = pl.BlockSpec(memory_space=pltpu.VMEM)
    exchange = pltpu.VMEM((sections, pieces * cap, part), bf16)
    stream_out, kv_t = pl.pallas_call(
        functools.partial(kernel, sections, cap, pieces),
        out_shape=(
            jax.ShapeDtypeStruct((tokens, model), bf16),
            jax.ShapeDtypeStruct((width, NX * NZ * 2 * tokens), bf16),
        ),
        in_specs=[vmem] * 4 + [any_space] * 3 + [vmem, any_space],
        out_specs=(vmem, vmem),
        scratch_shapes=[
            pltpu.VMEM((NX, NZ, 2, rows, model), bf16),
            pltpu.VMEM((NX, NZ, 2, rows, model), bf16),
            pltpu.VMEM((hidden, model), bf16),
            pltpu.VMEM((hidden, model), bf16),
            pltpu.VMEM((hidden, model), bf16),
            pltpu.VMEM((8 * rows, hidden), bf16),
            pltpu.VMEM((4, 4, rows, model), bf16),
            pltpu.VMEM((2, 4, rows, model), bf16),
            pltpu.VMEM((4, rows, model), bf16),
            pltpu.VMEM((3, rows, model), bf16),
            pltpu.VMEM((3, rows, 2 * mid_of(model)), bf16),
            exchange,
            exchange,
            exchange,
            pltpu.VMEM((NX, 2, tokens, model), bf16),
            pltpu.VMEM((NZ, width, model), bf16),
            pltpu.VMEM((NZ, width, NX * 2 * tokens), bf16),
            pltpu.VMEM((NZ, width, NX * 2 * tokens), bf16),
            dma((4,)),
            dma((8,)), dma((8,)), dma((8,)), dma((8,)),
            dma((4,)), dma((4,)),
            dma((3,)), dma((3,)), dma((3, 3)), dma((3, 3)),
            dma((2,)), dma((2,)), dma((2,)), dma((2,)), dma((4,)), dma((4,)),
            *Gather.sems(),
            *Reduce.sems(),
        ],
        compiler_params=pltpu.CompilerParams(
            collective_id=0, has_side_effects=True, vmem_limit_bytes=VMEM_LIMIT
        ),
        name="layer",
    )(
        stream, ffn_gain[None, :], router_weight.T, expert_ids.T,
        jnp.swapaxes(w_gate, 1, 2), jnp.swapaxes(w_up, 1, 2), w_down, attn_gain[None, :], w_kv.T,
    )
    return (stream_out, kv_t.T)


def solution(mesh):
    in_specs = (
        P(("section", "mp"), None),
        P(),
        P(),
        P(("section", "mp"), None),
        P("section", None, "mp"),
        P("section", None, "mp"),
        P("section", "mp", None),
        P(),
        P(None, "mp"),
    )
    out_specs = (P(("section", "mp"), None), P("section", "mp"))
    return jax.shard_map(body, mesh=mesh, in_specs=in_specs, out_specs=out_specs, check_vma=False)
```
